32 devices in a mesh: grp: 4 (over z), lane: 8 (over y, x, core).
Axes of the slice: x: 2, y: 2, z: 4, core: 2. Of those that a mesh axis runs over, the one named last changes fastest.
Arguments:
- factor_left: float32 [1048576], P(('grp', 'lane')), may hold values from -7 to 7, as said below
- denom_right: float32 [1048576], P(('grp', 'lane')), may hold values from -7 to 7, as said below
- bessel_left: float32 [1048576], P(('grp', 'lane')), may hold values from -7 to 7, as said below
- bessel_right: float32 [1048576], P(('grp', 'lane')), may hold values from -7 to 7, as said below
- harmonic_left: float32 [1048576], P(('grp', 'lane')), may hold values from -7 to 7, as said below
- harmonic_right: float32 [1048576], P(('grp', 'lane')), may hold values from -7 to 7, as said below
- weighted_left: float32 [1048576], P(('grp', 'lane')), may hold values from -7 to 7, as said below
Outputs:
- bessel_sum: float32 [2097152], P(('grp', 'lane'))
- harmonic_sum: float32 [2097152], P(('grp', 'lane'))
The draws below stay inside these ranges and needn't reach their ends.
Inputs may be any that keep to these rules, and one draw needn't show every extreme that they name: `factor_left`: every limb is a whole number. `denom_right`: every limb is a whole number. `bessel_left`: every limb is a whole number. `bessel_right`: every limb is a whole number. `harmonic_left`: every limb is a whole number. `harmonic_right`: every limb is a whole number. `weighted_left`: every limb is a whole number.
All inputs are finite; a program needn't handle non-finite values.
Results may differ from the reference program's by a relative error of at most 0.00045.
Values sent between devices are 32-bit elements; how exact they have to be, the bound alone decides.
No kernel may reach another device: no remote copies, remote signals or barrier semaphores. Data moves between devices by JAX's collectives and lax.ppermute only.
A program may use at most 128 MiB of HBM per device.

```python
import jax
import jax.numpy as jnp
from jax import lax

LIMB_DEV = 32768
LIMBS = 1048576


def limb_draw(key, salt):
    return jax.random.randint(jax.random.fold_in(key, salt), (LIMBS,), -7, 8).astype(jnp.float32)


def draw_factor_left(key, part):
    return limb_draw(key, 101)


def draw_denom_right(key, part):
    return limb_draw(key, 202)


def draw_bessel_left(key, part):
    return limb_draw(key, 303)


def draw_bessel_right(key, part):
    return limb_draw(key, 404)


def draw_harmonic_left(key, part):
    return limb_draw(key, 505)


def draw_harmonic_right(key, part):
    return limb_draw(key, 606)


def draw_weighted_left(key, part):
    return limb_draw(key, 707)


def setup_inputs(seed: int = 0) -> dict:
    seeds = jax.random.split(jax.random.key(seed), 8)
    factor_left = draw_factor_left(jax.random.fold_in(seeds[7], 71), 0)
    denom_right = draw_denom_right(jax.random.fold_in(seeds[7], 71), 0)
    bessel_left = draw_bessel_left(jax.random.fold_in(seeds[7], 71), 0)
    bessel_right = draw_bessel_right(jax.random.fold_in(seeds[7], 71), 0)
    harmonic_left = draw_harmonic_left(jax.random.fold_in(seeds[7], 71), 0)
    harmonic_right = draw_harmonic_right(jax.random.fold_in(seeds[7], 71), 0)
    weighted_left = draw_weighted_left(jax.random.fold_in(seeds[7], 71), 0)
    return dict(factor_left=factor_left, denom_right=denom_right, bessel_left=bessel_left, bessel_right=bessel_right, harmonic_left=harmonic_left, harmonic_right=harmonic_right, weighted_left=weighted_left)


def combine(earlier, later):
    return (earlier[0] * later[0], earlier[1] * later[0] + later[1])

def carried(values):
    rates = jnp.full(values.shape, jnp.exp(jnp.float32(-1.0 / (2 * LIMB_DEV))), dtype=jnp.float32)
    return lax.associative_scan(combine, (rates, values))[1]

def reference(factor_left, denom_right, bessel_left, bessel_right, harmonic_left, harmonic_right, weighted_left):
    padded = 2 * LIMBS

    def spectrum(limbs):
        return jnp.fft.rfft(limbs, padded)
    factor_spec = spectrum(factor_left)
    denom_spec = spectrum(denom_right)
    bessel_left_spec = spectrum(bessel_left)
    bessel_right_spec = spectrum(bessel_right)
    harmonic_left_spec = spectrum(harmonic_left)
    harmonic_right_spec = spectrum(harmonic_right)
    weighted_spec = spectrum(weighted_left)
    scaling = 1.0 / (16.0 * jnp.sqrt(jnp.float32(LIMBS)) * jnp.sqrt(jnp.float32(LIMB_DEV)))
    bessel = jnp.fft.irfft(bessel_left_spec * denom_spec + factor_spec * bessel_right_spec, padded) * scaling
    harmonic = jnp.fft.irfft(harmonic_left_spec * denom_spec + factor_spec * harmonic_right_spec + weighted_spec * bessel_right_spec, padded) * scaling
    return (carried(bessel.astype(jnp.float32)), carried(harmonic.astype(jnp.float32)))
```

```python
import math

import jax
import jax.numpy as jnp
import numpy as np
from jax import lax
from jax.experimental import pallas as pl
from jax.experimental.pallas import tpu as pltpu
from jax.sharding import PartitionSpec as P

AXES = ("grp", "lane")
LANES = 128
FWD_OPS = 7
VMEM = pltpu.MemorySpace.VMEM


def device_count():
    return lax.axis_size("grp") * lax.axis_size("lane")


def device_position():
    return lax.axis_index("grp") * lax.axis_size("lane") + lax.axis_index("lane")


def turn(numer, denom):
    reduced = numer % denom
    reduced = jnp.where(2 * reduced > denom, reduced - denom, reduced)
    angle = reduced.astype(jnp.float32) * (2.0 * math.pi / denom)
    return jnp.cos(angle), jnp.sin(angle)


def split16(value):
    high = value.astype(jnp.bfloat16)
    return high, (value - high.astype(jnp.float32)).astype(jnp.bfloat16)


def split_table(value):
    high = lax.reduce_precision(value, 8, 7)
    return high.astype(jnp.bfloat16), (value - high).astype(jnp.bfloat16)


def dot3(left, right):
    out = jnp.dot(left[0], right[1], preferred_element_type=jnp.float32)
    out += jnp.dot(left[1], right[0], preferred_element_type=jnp.float32)
    return out + jnp.dot(left[0], right[0], preferred_element_type=jnp.float32)


def tree_forward(values, numer, denom, emit):
    if len(values) == 1:
        emit(numer, denom, values[0])
        return
    half = len(values) // 2
    numer, denom = numer, 2 * denom
    cos, sin = math.cos(2 * math.pi * numer / denom), math.sin(2 * math.pi * numer / denom)
    plus, minus = [], []
    for low, high in zip(values[:half], values[half:]):
        if low[1] is None:
            re, im = cos * high[0], sin * high[0]
            plus.append((low[0] + re, im))
            minus.append((low[0] - re, -im))
        else:
            re = cos * high[0] - sin * high[1]
            im = sin * high[0] + cos * high[1]
            plus.append((low[0] + re, low[1] + im))
            minus.append((low[0] - re, low[1] - im))
    tree_forward(plus, numer, denom, emit)
    tree_forward(minus, numer + denom // 2, denom, emit)


def tree_inverse(size, numer, denom, load):
    if size == 1:
        return [load(numer, denom)]
    denom = 2 * denom
    cos, sin = math.cos(2 * math.pi * numer / denom), math.sin(2 * math.pi * numer / denom)
    plus = tree_inverse(size // 2, numer, denom, load)
    minus = tree_inverse(size // 2, numer + denom // 2, denom, load)
    low = [(a[0] + b[0], a[1] + b[1]) for a, b in zip(plus, minus)]
    high = []
    for a, b in zip(plus, minus):
        re, im = a[0] - b[0], a[1] - b[1]
        high.append((cos * re + sin * im, cos * im - sin * re))
    return low + high


def slot_of(numer, denom, devices):
    numer = (numer * (4 * devices // denom)) % (4 * devices)
    return (numer - 1) // 4


def spread_kernel(x_ref, out_ref):
    devices = x_ref.shape[0]

    def one(op, carry):
        values = [(x_ref[d, op], None) for d in range(devices)]

        def emit(numer, denom, value):
            slot = slot_of(numer, denom, devices)
            out_ref[slot, op, 0] = value[0]
            out_ref[slot, op, 1] = value[1]

        tree_forward(values, 1, 4, emit)
        return carry

    lax.fori_loop(0, x_ref.shape[1], one, 0)


def gather_kernel(u_ref, out_ref):
    devices = u_ref.shape[0]
    for out in range(u_ref.shape[1]):

        def load(numer, denom):
            slot = slot_of(numer, denom, devices)
            return u_ref[slot, out, 0], u_ref[slot, out, 1]

        for block, (re, im) in enumerate(tree_inverse(devices, 1, 4, load)):
            out_ref[block // 2, out, block % 2] = re
            out_ref[(devices + block) // 2, out, (devices + block) % 2] = im


def spectrum_kernel(x_ref, a_hi, a_lo, turn_ref, b_ref, h_ref, ai_hi, ai_lo, out_ref, spec_ref):
    rows = turn_ref.shape[1]
    turn_re, turn_im = turn_ref[0], turn_ref[1]
    table = (a_hi[...], a_lo[...])
    table_inv = (ai_hi[...], ai_lo[...])
    lane_table = (b_ref[0], b_ref[1])
    lane_table_inv = (b_ref[2], b_ref[3])

    def column_stage(stage_table, re, im):
        both = dot3(stage_table, split16(jnp.concatenate([re, im], axis=1)))
        top, bottom = both[:rows], both[rows:]
        return top[:, :LANES] - bottom[:, LANES:], top[:, LANES:] + bottom[:, :LANES]

    def forward(op, carry):
        re, im = column_stage(
            table, x_ref[:, op, 0].reshape(rows, LANES), x_ref[:, op, 1].reshape(rows, LANES)
        )
        turned = jnp.concatenate(
            [re * turn_re - im * turn_im, re * turn_im + im * turn_re], axis=1
        )
        spec_ref[op] = dot3(split16(turned), lane_table)
        return carry

    lax.fori_loop(0, FWD_OPS, forward, 0)

    def member(op):
        return spec_ref[op, :, :LANES], spec_ref[op, :, LANES:]

    def products(pairs):
        re, im = 0.0, 0.0
        for left, right in pairs:
            left_re, left_im = member(left)
            right_re, right_im = member(right)
            re = re + (left_re * right_re - left_im * right_im)
            im = im + (left_re * right_im + left_im * right_re)
        return re, im

    for out, pairs in enumerate((((2, 1), (0, 3)), ((4, 1), (0, 5), (6, 3)))):
        re, im = products(pairs)
        h_re, h_im = h_ref[0], h_ref[1]
        damped = jnp.concatenate([re * h_re - im * h_im, re * h_im + im * h_re], axis=1)
        both = dot3(split16(damped), lane_table_inv)
        re, im = both[:, :LANES], both[:, LANES:]
        re, im = re * turn_re + im * turn_im, im * turn_re - re * turn_im
        re, im = column_stage(table_inv, re, im)
        piece = (out_ref.shape[0],) + out_ref.shape[3:]
        out_ref[:, out, 0] = re.reshape(piece)
        out_ref[:, out, 1] = im.reshape(piece)


def call(kernel, out_shape, *args, scratch=()):
    return pl.pallas_call(
        kernel,
        out_shape=jax.ShapeDtypeStruct(out_shape, jnp.float32),
        in_specs=[pl.BlockSpec(memory_space=VMEM)] * len(args),
        out_specs=pl.BlockSpec(memory_space=VMEM),
        scratch_shapes=scratch,
    )(*args)


def exchange(value):
    return lax.all_to_all(value, AXES, split_axis=0, concat_axis=0, tiled=True)


def lane_tables():
    index = np.arange(LANES)
    angle = 2.0 * np.pi * ((index[:, None] * index[None, :]) % LANES) / LANES
    cos, sin = np.cos(angle), np.sin(angle)
    forward = np.block([[cos, sin], [-sin, cos]]).astype(np.float32)
    backward = np.block([[cos, -sin], [sin, cos]]).astype(np.float32)
    parts = []
    for table in (forward, backward):
        high = table.astype(jnp.bfloat16)
        parts += [high, (table - high.astype(np.float32)).astype(jnp.bfloat16)]
    return jnp.asarray(np.stack(parts))


def tables(local_limbs, devices, scaling, rate):
    rows = local_limbs // LANES
    period = 4 * local_limbs * devices
    freq = 4 * device_position() + 1

    def grid(shape):
        return (lax.broadcasted_iota(jnp.int32, shape, 0), lax.broadcasted_iota(jnp.int32, shape, 1))

    q1, t1 = grid((rows, rows))
    step = period // rows
    cos, sin = turn(((t1 * q1) % rows) * step + LANES * t1 * freq, period)
    forward = split_table(jnp.concatenate([cos, sin], axis=0))
    t1, q1 = grid((rows, rows))
    cos, sin = turn(((t1 * q1) % rows) * step + LANES * t1 * freq, period)
    backward = split_table(jnp.concatenate([cos, -sin], axis=0))
    q1, t2 = grid((rows, LANES))
    between = jnp.stack(turn(t2 * (q1 * (period // local_limbs) + freq), period))
    numer = freq + 4 * devices * (q1 + rows * t2)
    numer = jnp.where(2 * numer > period, numer - period, numer)
    angle = numer.astype(jnp.float32) * (2.0 * math.pi / period)
    half = jnp.sin(0.5 * angle)
    damp = math.exp(-rate)
    den_re = -math.expm1(-rate) + (2.0 * damp) * half * half
    den_im = -damp * jnp.sin(angle)
    norm = scaling / (den_re * den_re + den_im * den_im)
    filt = jnp.stack([den_re * norm, -den_im * norm])
    return forward, between, filt, backward


def damped_totals(stacked, rate, scaling):
    devices = device_count()
    local_limbs = stacked.shape[0] * stacked.shape[2] * LANES
    shape = (stacked.shape[0], 1, stacked.shape[2], LANES)
    index = (
        lax.broadcasted_iota(jnp.int32, shape, 0) * shape[2]
        + lax.broadcasted_iota(jnp.int32, shape, 2)
    ) * LANES + lax.broadcasted_iota(jnp.int32, shape, 3)
    left = (local_limbs - 1 - index) + (devices - 1 - device_position()) * local_limbs
    sums = jnp.sum(stacked * jnp.exp(left.astype(jnp.float32) * -rate), axis=(0, 2, 3))
    step = 1
    while step < devices:
        pairs = [(d, d ^ step) for d in range(devices)]
        sums = sums + lax.ppermute(sums, AXES, pairs)
        step *= 2
    factor = scaling * math.exp(-rate)
    return (
        factor * (sums[2] * sums[1] + sums[0] * sums[3]),
        factor * (sums[4] * sums[1] + sums[0] * sums[5] + sums[6] * sums[3]),
    )


def local(*operands):
    devices = device_count()
    local_limbs = operands[0].shape[0]
    total = local_limbs * devices
    rate = 1.0 / (2 * local_limbs)
    scaling = 1.0 / (16.0 * math.sqrt(total) * math.sqrt(local_limbs))
    rows = local_limbs // LANES
    piece = rows // devices
    inside = piece % 8 == 0

    stacked = jnp.stack([v.reshape(devices, piece, LANES) for v in operands], axis=1)
    received = exchange(stacked)
    ends = damped_totals(stacked, rate, scaling)
    forward, between, filt, backward = tables(local_limbs, devices, scaling / total, rate)

    spread = call(spread_kernel, (devices, FWD_OPS, 2, piece, LANES), received)
    landed = exchange(spread)
    if not inside:
        landed = landed.transpose(1, 2, 0, 3, 4).reshape(1, FWD_OPS, 2, rows, LANES)
    out_piece = (devices, 2, 2, piece, LANES) if inside else (1, 2, 2, rows, LANES)
    turned = call(
        spectrum_kernel,
        out_piece,
        landed,
        *forward,
        between,
        lane_tables(),
        filt,
        *backward,
        scratch=[pltpu.VMEM((FWD_OPS, rows, 2 * LANES), jnp.float32)],
    )
    if not inside:
        turned = turned.reshape(2, 2, devices, piece, LANES).transpose(2, 0, 1, 3, 4)
    gathered = exchange(turned)
    coeffs = call(gather_kernel, (devices, 2, 2, piece, LANES), gathered)
    owned = exchange(coeffs)

    results = []
    for out in range(2):
        mine = owned[:, out].transpose(1, 0, 2, 3).reshape(2 * local_limbs)
        index = lax.broadcasted_iota(jnp.int32, (2 * local_limbs,), 0)
        index = index + device_position() * (2 * local_limbs)
        decay = jnp.exp((index + 1).astype(jnp.float32) * -rate)
        results.append(mine + ends[out] * decay)
    return tuple(results)


def solution(mesh):
    return jax.shard_map(
        local,
        mesh=mesh,
        in_specs=(P(AXES),) * FWD_OPS,
        out_specs=(P(AXES), P(AXES)),
        check_vma=False,
    )
```

```python
import math

import jax
import jax.numpy as jnp
import numpy as np
from jax import lax
from jax.experimental import pallas as pl
from jax.experimental.pallas import tpu as pltpu
from jax.sharding import PartitionSpec as P

AXES = ("grp", "lane")
LANES = 128
FWD_OPS = 7
CARRY_ROWS = 4
VMEM = pltpu.MemorySpace.VMEM


def device_count():
    return lax.axis_size("grp") * lax.axis_size("lane")


def device_position():
    return lax.axis_index("grp") * lax.axis_size("lane") + lax.axis_index("lane")


def turn(numer, denom):
    reduced = numer % denom
    reduced = jnp.where(2 * reduced > denom, reduced - denom, reduced)
    angle = reduced.astype(jnp.float32) * (2.0 * math.pi / denom)
    return jnp.cos(angle), jnp.sin(angle)


def split16(value):
    high = value.astype(jnp.bfloat16)
    return high, (value - high.astype(jnp.float32)).astype(jnp.bfloat16)


def split_table(value):
    high = lax.reduce_precision(value, 8, 7)
    return high.astype(jnp.bfloat16), (value - high).astype(jnp.bfloat16)


def wide_left(parts):
    return jnp.concatenate([parts[0], parts[1], parts[0]], axis=1)


def tall_right(parts):
    return jnp.concatenate([parts[0], parts[0], parts[1]], axis=0)


def dot32(left, right):
    return jnp.dot(left, right, preferred_element_type=jnp.float32)


def tree_forward(values, numer, denom, emit):
    if len(values) == 1:
        emit(numer, denom, values[0])
        return
    half = len(values) // 2
    numer, denom = numer, 2 * denom
    cos, sin = math.cos(2 * math.pi * numer / denom), math.sin(2 * math.pi * numer / denom)
    plus, minus = [], []
    for low, high in zip(values[:half], values[half:]):
        if low[1] is None:
            re, im = cos * high[0], sin * high[0]
            plus.append((low[0] + re, im))
            minus.append((low[0] - re, -im))
        else:
            re = cos * high[0] - sin * high[1]
            im = sin * high[0] + cos * high[1]
            plus.append((low[0] + re, low[1] + im))
            minus.append((low[0] - re, low[1] - im))
    tree_forward(plus, numer, denom, emit)
    tree_forward(minus, numer + denom // 2, denom, emit)


def tree_inverse(size, numer, denom, load):
    if size == 1:
        return [load(numer, denom)]
    denom = 2 * denom
    cos, sin = math.cos(2 * math.pi * numer / denom), math.sin(2 * math.pi * numer / denom)
    plus = tree_inverse(size // 2, numer, denom, load)
    minus = tree_inverse(size // 2, numer + denom // 2, denom, load)
    low = [(a[0] + b[0], a[1] + b[1]) for a, b in zip(plus, minus)]
    high = []
    for a, b in zip(plus, minus):
        re, im = a[0] - b[0], a[1] - b[1]
        high.append((cos * re + sin * im, cos * im - sin * re))
    return low + high


def slot_of(numer, denom, devices):
    numer = (numer * (4 * devices // denom)) % (4 * devices)
    return (numer - 1) // 4


def spread_kernel(x_ref, out_far, out_ref, sems):
    devices = x_ref.shape[0]
    copies = []
    for op in range(FWD_OPS):
        values = [(x_ref[d, op], None) for d in range(devices)]

        def emit(numer, denom, value):
            slot = slot_of(numer, denom, devices)
            out_ref[op, slot, 0] = value[0]
            out_ref[op, slot, 1] = value[1]

        tree_forward(values, 1, 4, emit)
        copies.append(pltpu.make_async_copy(out_ref.at[op], out_far.at[:, op], sems.at[op]))
        copies[-1].start()
    for copy in copies:
        copy.wait()


def gather_kernel(u_ref, last_ref, decay_ref, out_ref):
    devices = u_ref.shape[0]
    rows = decay_ref.shape[0]
    packed = len(u_ref.shape) == 4
    for out in range(2):

        def part(slot, which):
            if not packed:
                return u_ref[slot, out, which]
            groups = rows // CARRY_ROWS
            first = (2 * out + which) * groups
            return jnp.concatenate([u_ref[slot, first + k] for k in range(groups)], axis=0)

        def last(slot, which):
            row = 2 * out + which
            ref = u_ref.at[slot, u_ref.shape[1] - 1] if packed else last_ref.at[slot]
            return ref[row : row + 1]

        wrap = 0.0
        for slot in range(devices):
            angle = 2.0 * math.pi * ((devices - 1) * (4 * slot + 1)) / (4 * devices)
            wrap = wrap + (math.cos(angle) * last(slot, 1) - math.sin(angle) * last(slot, 0))
        lane = lax.broadcasted_iota(jnp.int32, wrap.shape, 1)
        wrap = jnp.sum(jnp.where(lane == LANES - 1, wrap, 0.0), axis=1, keepdims=True)
        tail = decay_ref[...] * wrap

        def load(numer, denom):
            slot = slot_of(numer, denom, devices)
            return part(slot, 0), part(slot, 1)

        for block, pair in enumerate(tree_inverse(devices, 1, 4, load)):
            for k, value in enumerate(pair):
                index = k * devices + block
                value = value + math.exp(-0.5 * index) * tail
                out_ref[index // 2, out, index % 2] = value


def copy_all(pairs, sems):
    copies = [pltpu.make_async_copy(a, b, sems.at[k]) for k, (a, b) in enumerate(pairs)]
    for copy in copies:
        copy.start()
    return copies


def stack_kernel(*refs):
    operands, out_ref, sems = refs[:-2], refs[-2], refs[-1]
    pairs = [(ref, out_ref.at[:, op]) for op, ref in enumerate(operands)]
    for copy in copy_all(pairs, sems):
        copy.wait()


def deliver_kernel(in_ref, first_ref, second_ref, sems):
    pairs = [
        (in_ref.at[:, out, half], ref.at[half])
        for out, ref in enumerate((first_ref, second_ref))
        for half in range(2)
    ]
    for copy in copy_all(pairs, sems):
        copy.wait()


def spectrum_kernel(
    x_ref, a_ref, turn_ref, b_ref, h_far, ai_far, out_ref, spec_ref, h_ref, ai_ref, sems
):
    rows = turn_ref.shape[1]
    copies = copy_all([(h_far, h_ref), (ai_far, ai_ref)], sems)

    def column_stage(table_ref, re, im):
        both = dot32(table_ref[...], tall_right(split16(jnp.concatenate([re, im], axis=1))))
        top, bottom = both[:rows], both[rows:]
        return top[:, :LANES] - bottom[:, LANES:], top[:, LANES:] + bottom[:, :LANES]

    for op in range(FWD_OPS):
        re, im = column_stage(
            a_ref, x_ref[:, op, 0].reshape(rows, LANES), x_ref[:, op, 1].reshape(rows, LANES)
        )
        turn_re, turn_im = turn_ref[0], turn_ref[1]
        turned = jnp.concatenate(
            [re * turn_re - im * turn_im, re * turn_im + im * turn_re], axis=1
        )
        spec_ref[op] = dot32(wide_left(split16(turned)), b_ref[0])

    for copy in copies:
        copy.wait()

    def store(out, which, value):
        if len(out_ref.shape) == 5:
            out_ref[:, out, which] = value.reshape((out_ref.shape[0],) + out_ref.shape[3:])
            return
        devices = out_ref.shape[0]
        groups = rows // devices // CARRY_ROWS
        value = value.reshape(devices, groups * CARRY_ROWS, LANES)
        for k in range(groups):
            part = value[:, k * CARRY_ROWS : (k + 1) * CARRY_ROWS]
            out_ref[:, (2 * out + which) * groups + k] = part
        row = value[devices - 1 :, groups * CARRY_ROWS - 1 :]
        out_ref[:, 4 * groups, pl.ds(2 * out + which, 1)] = jnp.broadcast_to(
            row, (devices, 1, LANES)
        ).reshape(devices, 1, LANES)

    def member(op):
        return spec_ref[op, :, :LANES], spec_ref[op, :, LANES:]

    def products(pairs):
        re, im = 0.0, 0.0
        for left, right in pairs:
            left_re, left_im = member(left)
            right_re, right_im = member(right)
            re = re + (left_re * right_re - left_im * right_im)
            im = im + (left_re * right_im + left_im * right_re)
        return re, im

    for out, pairs in enumerate((((2, 1), (0, 3)), ((4, 1), (0, 5), (6, 3)))):
        re, im = products(pairs)
        h_re, h_im = h_ref[0], h_ref[1]
        damped = jnp.concatenate([re * h_re - im * h_im, re * h_im + im * h_re], axis=1)
        both = dot32(wide_left(split16(damped)), b_ref[1])
        re, im = both[:, :LANES], both[:, LANES:]
        turn_re, turn_im = turn_ref[0], turn_ref[1]
        re, im = re * turn_re + im * turn_im, im * turn_re - re * turn_im
        re, im = column_stage(ai_ref, re, im)
        for which, value in enumerate((re, im)):
            store(out, which, value)


def call(kernel, name, out_shapes, *args, near, scratch=()):
    spaces = [VMEM if flag else pltpu.MemorySpace.HBM for flag in near]
    args = [pltpu.with_memory_space_constraint(v, space) for v, space in zip(args, spaces)]
    specs = [pl.BlockSpec(memory_space=space) for space in spaces]
    outs = [space(shape, jnp.float32) for shape, space in zip(out_shapes, spaces[len(args) :])]
    return pl.pallas_call(
        kernel,
        out_shape=outs,
        in_specs=specs[: len(args)],
        out_specs=specs[len(args) :],
        scratch_shapes=scratch,
        compiler_params=pltpu.CompilerParams(vmem_limit_bytes=24 << 20),
        name=name,
    )(*args)


def exchange(value):
    return lax.all_to_all(value, AXES, split_axis=0, concat_axis=0, tiled=True)


def lane_tables():
    index = np.arange(LANES)
    angle = 2.0 * np.pi * ((index[:, None] * index[None, :]) % LANES) / LANES
    cos, sin = np.cos(angle), np.sin(angle)
    forward = np.block([[cos, sin], [-sin, cos]]).astype(np.float32)
    backward = np.block([[cos, -sin], [sin, cos]]).astype(np.float32)
    parts = []
    for table in (forward, backward):
        high = table.astype(jnp.bfloat16)
        low = (table - high.astype(np.float32)).astype(jnp.bfloat16)
        parts.append(np.concatenate([high, high, low], axis=0))
    return jnp.asarray(np.stack(parts))


def tables(local_limbs, devices, scaling, rate):
    rows = local_limbs // LANES
    period = 4 * local_limbs * devices
    freq = 4 * device_position() + 1

    def grid(shape):
        return (lax.broadcasted_iota(jnp.int32, shape, 0), lax.broadcasted_iota(jnp.int32, shape, 1))

    q1, t1 = grid((rows, rows))
    step = period // rows
    cos, sin = turn(((t1 * q1) % rows) * step + LANES * t1 * freq, period)
    forward = wide_left(split_table(jnp.concatenate([cos, sin], axis=0)))
    t1, q1 = grid((rows, rows))
    cos, sin = turn(((t1 * q1) % rows) * step + LANES * t1 * freq, period)
    backward = wide_left(split_table(jnp.concatenate([cos, -sin], axis=0)))
    q1, t2 = grid((rows, LANES))
    between = jnp.stack(turn(t2 * (q1 * (period // local_limbs) + freq), period))
    numer = freq + 4 * devices * (q1 + rows * t2)
    numer = jnp.where(2 * numer > period, numer - period, numer)
    angle = numer.astype(jnp.float32) * (2.0 * math.pi / period)
    half = jnp.sin(0.5 * angle)
    damp = math.exp(-rate)
    den_re = -math.expm1(-rate) + (2.0 * damp) * half * half
    den_im = -damp * jnp.sin(angle)
    norm = scaling / (den_re * den_re + den_im * den_im)
    filt = jnp.stack([den_re * norm, -den_im * norm])
    return forward, between, filt, backward


def local(*operands):
    devices = device_count()
    local_limbs = operands[0].shape[0]
    total = local_limbs * devices
    rate = 1.0 / (2 * local_limbs)
    scaling = 1.0 / (16.0 * math.sqrt(total) * math.sqrt(local_limbs))
    rows = local_limbs // LANES
    piece = rows // devices
    inside = piece % 8 == 0

    dma = pltpu.SemaphoreType.DMA
    far_ops = [v.reshape(devices, piece, LANES) for v in operands]
    (stacked,) = call(
        stack_kernel,
        "stack",
        [(devices, FWD_OPS, piece, LANES)],
        *far_ops,
        near=[False] * FWD_OPS + [True],
        scratch=[dma((FWD_OPS,))],
    )
    received = exchange(stacked)
    forward, between, filt, backward = tables(local_limbs, devices, scaling / total, rate)
    consts = (forward, between, lane_tables(), filt, backward)
    shape = (piece, LANES)
    index = (device_position() * piece + lax.broadcasted_iota(jnp.int32, shape, 0)) * LANES
    index = index + lax.broadcasted_iota(jnp.int32, shape, 1)
    decay = jnp.exp((index + 1).astype(jnp.float32) * -rate)

    (spread,) = call(
        spread_kernel,
        "spread",
        [(devices, FWD_OPS, 2, piece, LANES)],
        received,
        near=[True, False],
        scratch=[
            pltpu.VMEM((FWD_OPS, devices, 2, piece, LANES), jnp.float32),
            dma((FWD_OPS,)),
        ],
    )
    landed = exchange(spread)
    if not inside:
        landed = landed.transpose(1, 2, 0, 3, 4).reshape(1, FWD_OPS, 2, rows, LANES)
    groups = 4 * piece // CARRY_ROWS
    packed = (devices, groups + 1, CARRY_ROWS, LANES)
    (turned,) = call(
        spectrum_kernel,
        "spectrum",
        [packed if inside else (1, 2, 2, rows, LANES)],
        landed,
        *consts,
        near=[True] * 4 + [False] * 2 + [True],
        scratch=[
            pltpu.VMEM((FWD_OPS, rows, 2 * LANES), jnp.float32),
            pltpu.VMEM(filt.shape, filt.dtype),
            pltpu.VMEM(backward.shape, backward.dtype),
            dma((2,)),
        ],
    )
    if not inside:
        data = turned.reshape(4, devices, piece, LANES).transpose(1, 0, 2, 3)
        last = jnp.broadcast_to(turned[0, :, :, -1].reshape(1, 1, 4, LANES), (devices, 1, 4, LANES))
        turned = jnp.concatenate([data.reshape(devices, groups, CARRY_ROWS, LANES), last], axis=1)
    gathered = exchange(turned)
    last = gathered[:, groups] if not inside else decay
    if not inside:
        gathered = gathered[:, :groups].reshape(devices, 2, 2, piece, LANES)
    (coeffs,) = call(
        gather_kernel,
        "gather",
        [(devices, 2, 2, piece, LANES)],
        gathered,
        last,
        decay,
        near=[True] * 4,
    )
    owned = exchange(coeffs)
    results = call(
        deliver_kernel,
        "deliver",
        [(2, devices, piece, LANES)] * 2,
        owned,
        near=[True, False, False],
        scratch=[dma((4,))],
    )
    return tuple(v.reshape(2 * local_limbs) for v in results)


def solution(mesh):
    return jax.shard_map(
        local,
        mesh=mesh,
        in_specs=(P(AXES),) * FWD_OPS,
        out_specs=(P(AXES), P(AXES)),
        check_vma=False,
    )
```

```python
import math

import jax
import jax.numpy as jnp
import numpy as np
from jax import lax
from jax.experimental import pallas as pl
from jax.experimental.pallas import tpu as pltpu
from jax.sharding import PartitionSpec as P

AXES = ("grp", "lane")
LANES = 128
FWD_OPS = 7
CARRY_ROWS = 4
VMEM = pltpu.MemorySpace.VMEM


def device_count():
    return lax.axis_size("grp") * lax.axis_size("lane")


def device_position():
    return lax.axis_index("grp") * lax.axis_size("lane") + lax.axis_index("lane")


def turn(numer, denom):
    reduced = numer % denom
    reduced = jnp.where(2 * reduced > denom, reduced - denom, reduced)
    angle = reduced.astype(jnp.float32) * (2.0 * math.pi / denom)
    return jnp.cos(angle), jnp.sin(angle)


def split16(value):
    high = value.astype(jnp.bfloat16)
    return high, (value - high.astype(jnp.float32)).astype(jnp.bfloat16)


def split_table(value):
    high = lax.reduce_precision(value, 8, 7)
    return high.astype(jnp.bfloat16), (value - high).astype(jnp.bfloat16)


def wide_left(parts):
    return jnp.concatenate([parts[0], parts[1], parts[0]], axis=1)


def tall_right(parts):
    return jnp.concatenate([parts[0], parts[0], parts[1]], axis=0)


def dot32(left, right):
    return jnp.dot(left, right, preferred_element_type=jnp.float32)


def tree_forward(values, numer, denom, emit):
    if len(values) == 1:
        emit(numer, denom, values[0])
        return
    half = len(values) // 2
    numer, denom = numer, 2 * denom
    cos, sin = math.cos(2 * math.pi * numer / denom), math.sin(2 * math.pi * numer / denom)
    plus, minus = [], []
    for low, high in zip(values[:half], values[half:]):
        if low[1] is None:
            re, im = cos * high[0], sin * high[0]
            plus.append((low[0] + re, im))
            minus.append((low[0] - re, -im))
        else:
            re = cos * high[0] - sin * high[1]
            im = sin * high[0] + cos * high[1]
            plus.append((low[0] + re, low[1] + im))
            minus.append((low[0] - re, low[1] - im))
    tree_forward(plus, numer, denom, emit)
    tree_forward(minus, numer + denom // 2, denom, emit)


def tree_inverse(size, numer, denom, load):
    if size == 1:
        return [load(numer, denom)]
    denom = 2 * denom
    cos, sin = math.cos(2 * math.pi * numer / denom), math.sin(2 * math.pi * numer / denom)
    plus = tree_inverse(size // 2, numer, denom, load)
    minus = tree_inverse(size // 2, numer + denom // 2, denom, load)
    low = [(a[0] + b[0], a[1] + b[1]) for a, b in zip(plus, minus)]
    high = []
    for a, b in zip(plus, minus):
        re, im = a[0] - b[0], a[1] - b[1]
        high.append((cos * re + sin * im, cos * im - sin * re))
    return low + high


def slot_of(numer, denom, devices):
    numer = (numer * (4 * devices // denom)) % (4 * devices)
    return (numer - 1) // 4


def spread_kernel(x_ref, out_far, out_ref, sems):
    devices = x_ref.shape[0]
    copies = []
    for op in range(FWD_OPS):
        values = [(x_ref[d, op], None) for d in range(devices)]

        def emit(numer, denom, value):
            slot = slot_of(numer, denom, devices)
            out_ref[op, slot, 0] = value[0]
            out_ref[op, slot, 1] = value[1]

        tree_forward(values, 1, 4, emit)
        copies.append(pltpu.make_async_copy(out_ref.at[op], out_far.at[:, op], sems.at[op]))
        copies[-1].start()
    for copy in copies:
        copy.wait()


def gather_kernel(u_ref, last_ref, decay_ref, out_ref):
    devices = u_ref.shape[0]
    rows = decay_ref.shape[0]
    packed = len(u_ref.shape) == 4
    for out in range(2):

        def part(slot, which):
            if not packed:
                return u_ref[slot, out, which]
            groups = rows // CARRY_ROWS
            first = (2 * out + which) * groups
            return jnp.concatenate([u_ref[slot, first + k] for k in range(groups)], axis=0)

        def last(slot, which):
            row = 2 * out + which
            ref = u_ref.at[slot, u_ref.shape[1] - 1] if packed else last_ref.at[slot]
            return ref[row : row + 1]

        wrap = 0.0
        for slot in range(devices):
            angle = 2.0 * math.pi * ((devices - 1) * (4 * slot + 1)) / (4 * devices)
            wrap = wrap + (math.cos(angle) * last(slot, 1) - math.sin(angle) * last(slot, 0))
        lane = lax.broadcasted_iota(jnp.int32, wrap.shape, 1)
        wrap = jnp.sum(jnp.where(lane == LANES - 1, wrap, 0.0), axis=1, keepdims=True)
        tail = decay_ref[...] * wrap

        def load(numer, denom):
            slot = slot_of(numer, denom, devices)
            return part(slot, 0), part(slot, 1)

        for block, pair in enumerate(tree_inverse(devices, 1, 4, load)):
            for k, value in enumerate(pair):
                index = k * devices + block
                value = value + math.exp(-0.5 * index) * tail
                out_ref[index // 2, out, index % 2] = value


def copy_all(pairs, sems):
    copies = [pltpu.make_async_copy(a, b, sems.at[k]) for k, (a, b) in enumerate(pairs)]
    for copy in copies:
        copy.start()
    return copies


def stack_kernel(*refs):
    operands, out_ref, sems = refs[:-2], refs[-2], refs[-1]
    pairs = [(ref, out_ref.at[:, op]) for op, ref in enumerate(operands)]
    for copy in copy_all(pairs, sems):
        copy.wait()


def deliver_kernel(in_ref, first_ref, second_ref, sems):
    pairs = [
        (in_ref.at[:, out, half], ref.at[half])
        for out, ref in enumerate((first_ref, second_ref))
        for half in range(2)
    ]
    for copy in copy_all(pairs, sems):
        copy.wait()


def spectrum_kernel(
    x_ref, a_ref, turn_ref, b_far, h_far, ai_far, out_ref,
    spec_ref, lhs_ref, b_ref, h_ref, ai_ref, sems,
):
    rows = turn_ref.shape[1]
    copies = copy_all([(b_far, b_ref), (h_far, h_ref), (ai_far, ai_ref)], sems)

    def column_stage(table_ref, re, im):
        both = dot32(table_ref[...], tall_right(split16(jnp.concatenate([re, im], axis=1))))
        top, bottom = both[:rows], both[rows:]
        return top[:, :LANES] - bottom[:, LANES:], top[:, LANES:] + bottom[:, :LANES]

    for op in range(FWD_OPS):
        re, im = column_stage(
            a_ref, x_ref[:, op, 0].reshape(rows, LANES), x_ref[:, op, 1].reshape(rows, LANES)
        )
        turn_re, turn_im = turn_ref[0], turn_ref[1]
        turned = jnp.concatenate(
            [re * turn_re - im * turn_im, re * turn_im + im * turn_re], axis=1
        )
        lhs_ref[op] = wide_left(split16(turned))

    for copy in copies:
        copy.wait()
    shape = spec_ref.shape
    left = lhs_ref[...].reshape(shape[0] * shape[1], lhs_ref.shape[2])
    spec_ref[...] = dot32(left, b_ref[0]).reshape(shape)

    def store(out, which, value):
        if len(out_ref.shape) == 5:
            out_ref[:, out, which] = value.reshape((out_ref.shape[0],) + out_ref.shape[3:])
            return
        devices = out_ref.shape[0]
        groups = rows // devices // CARRY_ROWS
        value = value.reshape(devices, groups * CARRY_ROWS, LANES)
        for k in range(groups):
            part = value[:, k * CARRY_ROWS : (k + 1) * CARRY_ROWS]
            out_ref[:, (2 * out + which) * groups + k] = part
        row = value[devices - 1 :, groups * CARRY_ROWS - 1 :]
        out_ref[:, 4 * groups, pl.ds(2 * out + which, 1)] = jnp.broadcast_to(
            row, (devices, 1, LANES)
        ).reshape(devices, 1, LANES)

    def member(op):
        return spec_ref[op, :, :LANES], spec_ref[op, :, LANES:]

    def products(pairs):
        re, im = 0.0, 0.0
        for left, right in pairs:
            left_re, left_im = member(left)
            right_re, right_im = member(right)
            re = re + (left_re * right_re - left_im * right_im)
            im = im + (left_re * right_im + left_im * right_re)
        return re, im

    for out, pairs in enumerate((((2, 1), (0, 3)), ((4, 1), (0, 5), (6, 3)))):
        re, im = products(pairs)
        h_re, h_im = h_ref[0], h_ref[1]
        damped = jnp.concatenate([re * h_re - im * h_im, re * h_im + im * h_re], axis=1)
        both = dot32(wide_left(split16(damped)), b_ref[1])
        re, im = both[:, :LANES], both[:, LANES:]
        turn_re, turn_im = turn_ref[0], turn_ref[1]
        re, im = re * turn_re + im * turn_im, im * turn_re - re * turn_im
        re, im = column_stage(ai_ref, re, im)
        for which, value in enumerate((re, im)):
            store(out, which, value)


def call(kernel, name, out_shapes, *args, near, scratch=()):
    spaces = [VMEM if flag else pltpu.MemorySpace.HBM for flag in near]
    args = [pltpu.with_memory_space_constraint(v, space) for v, space in zip(args, spaces)]
    specs = [pl.BlockSpec(memory_space=space) for space in spaces]
    outs = [space(shape, jnp.float32) for shape, space in zip(out_shapes, spaces[len(args) :])]
    return pl.pallas_call(
        kernel,
        out_shape=outs,
        in_specs=specs[: len(args)],
        out_specs=specs[len(args) :],
        scratch_shapes=scratch,
        compiler_params=pltpu.CompilerParams(vmem_limit_bytes=24 << 20),
        name=name,
    )(*args)


def exchange(value):
    return lax.all_to_all(value, AXES, split_axis=0, concat_axis=0, tiled=True)


def lane_tables():
    index = np.arange(LANES)
    angle = 2.0 * np.pi * ((index[:, None] * index[None, :]) % LANES) / LANES
    cos, sin = np.cos(angle), np.sin(angle)
    forward = np.block([[cos, sin], [-sin, cos]]).astype(np.float32)
    backward = np.block([[cos, -sin], [sin, cos]]).astype(np.float32)
    parts = []
    for table in (forward, backward):
        high = table.astype(jnp.bfloat16)
        low = (table - high.astype(np.float32)).astype(jnp.bfloat16)
        parts.append(np.concatenate([high, high, low], axis=0))
    return jnp.asarray(np.stack(parts))


def tables(local_limbs, devices, scaling, rate):
    rows = local_limbs // LANES
    period = 4 * local_limbs * devices
    freq = 4 * device_position() + 1

    def grid(shape):
        return (lax.broadcasted_iota(jnp.int32, shape, 0), lax.broadcasted_iota(jnp.int32, shape, 1))

    q1, t1 = grid((rows, rows))
    step = period // rows
    cos, sin = turn(((t1 * q1) % rows) * step + LANES * t1 * freq, period)
    forward = wide_left(split_table(jnp.concatenate([cos, sin], axis=0)))
    t1, q1 = grid((rows, rows))
    cos, sin = turn(((t1 * q1) % rows) * step + LANES * t1 * freq, period)
    backward = wide_left(split_table(jnp.concatenate([cos, -sin], axis=0)))
    q1, t2 = grid((rows, LANES))
    between = jnp.stack(turn(t2 * (q1 * (period // local_limbs) + freq), period))
    numer = freq + 4 * devices * (q1 + rows * t2)
    numer = jnp.where(2 * numer > period, numer - period, numer)
    angle = numer.astype(jnp.float32) * (2.0 * math.pi / period)
    half = jnp.sin(0.5 * angle)
    damp = math.exp(-rate)
    den_re = -math.expm1(-rate) + (2.0 * damp) * half * half
    den_im = -damp * jnp.sin(angle)
    norm = scaling / (den_re * den_re + den_im * den_im)
    filt = jnp.stack([den_re * norm, -den_im * norm])
    return forward, between, filt, backward


def local(*operands):
    devices = device_count()
    local_limbs = operands[0].shape[0]
    total = local_limbs * devices
    rate = 1.0 / (2 * local_limbs)
    scaling = 1.0 / (16.0 * math.sqrt(total) * math.sqrt(local_limbs))
    rows = local_limbs // LANES
    piece = rows // devices
    inside = piece % 8 == 0

    dma = pltpu.SemaphoreType.DMA
    far_ops = [v.reshape(devices, piece, LANES) for v in operands]
    (stacked,) = call(
        stack_kernel,
        "stack",
        [(devices, FWD_OPS, piece, LANES)],
        *far_ops,
        near=[False] * FWD_OPS + [True],
        scratch=[dma((FWD_OPS,))],
    )
    received = exchange(stacked)
    forward, between, filt, backward = tables(local_limbs, devices, scaling / total, rate)
    consts = (forward, between, lane_tables(), filt, backward)
    shape = (piece, LANES)
    index = (device_position() * piece + lax.broadcasted_iota(jnp.int32, shape, 0)) * LANES
    index = index + lax.broadcasted_iota(jnp.int32, shape, 1)
    decay = jnp.exp((index + 1).astype(jnp.float32) * -rate)

    (spread,) = call(
        spread_kernel,
        "spread",
        [(devices, FWD_OPS, 2, piece, LANES)],
        received,
        near=[True, False],
        scratch=[
            pltpu.VMEM((FWD_OPS, devices, 2, piece, LANES), jnp.float32),
            dma((FWD_OPS,)),
        ],
    )
    landed = exchange(spread)
    if not inside:
        landed = landed.transpose(1, 2, 0, 3, 4).reshape(1, FWD_OPS, 2, rows, LANES)
    groups = 4 * piece // CARRY_ROWS
    packed = (devices, groups + 1, CARRY_ROWS, LANES)
    (turned,) = call(
        spectrum_kernel,
        "spectrum",
        [packed if inside else (1, 2, 2, rows, LANES)],
        landed,
        *consts,
        near=[True] * 3 + [False] * 3 + [True],
        scratch=[
            pltpu.VMEM((FWD_OPS, rows, 2 * LANES), jnp.float32),
            pltpu.VMEM((FWD_OPS, rows, 6 * LANES), jnp.bfloat16),
        ]
        + [pltpu.VMEM(v.shape, v.dtype) for v in consts[2:]]
        + [dma((3,))],
    )
    if not inside:
        data = turned.reshape(4, devices, piece, LANES).transpose(1, 0, 2, 3)
        last = jnp.broadcast_to(turned[0, :, :, -1].reshape(1, 1, 4, LANES), (devices, 1, 4, LANES))
        turned = jnp.concatenate([data.reshape(devices, groups, CARRY_ROWS, LANES), last], axis=1)
    gathered = exchange(turned)
    last = gathered[:, groups] if not inside else decay
    if not inside:
        gathered = gathered[:, :groups].reshape(devices, 2, 2, piece, LANES)
    (coeffs,) = call(
        gather_kernel,
        "gather",
        [(devices, 2, 2, piece, LANES)],
        gathered,
        last,
        decay,
        near=[True] * 4,
    )
    owned = exchange(coeffs)
    results = call(
        deliver_kernel,
        "deliver",
        [(2, devices, piece, LANES)] * 2,
        owned,
        near=[True, False, False],
        scratch=[dma((4,))],
    )
    return tuple(v.reshape(2 * local_limbs) for v in results)


def solution(mesh):
    return jax.shard_map(
        local,
        mesh=mesh,
        in_specs=(P(AXES),) * FWD_OPS,
        out_specs=(P(AXES), P(AXES)),
        check_vma=False,
    )
```

```python
import functools
import math

import jax
import jax.numpy as jnp
import numpy as np
from jax import lax
from jax.experimental import pallas as pl
from jax.experimental.pallas import tpu as pltpu
from jax.sharding import PartitionSpec as P

AXES = ("grp", "lane")
LANES = 128
FWD_OPS = 7
VMEM = pltpu.MemorySpace.VMEM


def device_count():
    return lax.axis_size("grp") * lax.axis_size("lane")


def device_position():
    return lax.axis_index("grp") * lax.axis_size("lane") + lax.axis_index("lane")


def turn(numer, denom):
    reduced = numer % denom
    reduced = jnp.where(2 * reduced > denom, reduced - denom, reduced)
    angle = reduced.astype(jnp.float32) * (2.0 * math.pi / denom)
    return jnp.cos(angle), jnp.sin(angle)


def split16(value):
    high = value.astype(jnp.bfloat16)
    return high, (value - high.astype(jnp.float32)).astype(jnp.bfloat16)


def split_table(value):
    high = lax.reduce_precision(value, 8, 7)
    return high.astype(jnp.bfloat16), (value - high).astype(jnp.bfloat16)


def wide_left(parts):
    return jnp.concatenate([parts[0], parts[1], parts[0]], axis=1)


def tall_right(parts):
    return jnp.concatenate([parts[0], parts[0], parts[1]], axis=0)


def dot32(left, right):
    return jnp.dot(left, right, preferred_element_type=jnp.float32)


def tree_forward(values, numer, denom, emit):
    if len(values) == 1:
        emit(numer, denom, values[0])
        return
    half = len(values) // 2
    numer, denom = numer, 2 * denom
    cos, sin = math.cos(2 * math.pi * numer / denom), math.sin(2 * math.pi * numer / denom)
    plus, minus = [], []
    for low, high in zip(values[:half], values[half:]):
        if low[1] is None:
            re, im = cos * high[0], sin * high[0]
            plus.append((low[0] + re, im))
            minus.append((low[0] - re, -im))
        else:
            re = cos * high[0] - sin * high[1]
            im = sin * high[0] + cos * high[1]
            plus.append((low[0] + re, low[1] + im))
            minus.append((low[0] - re, low[1] - im))
    tree_forward(plus, numer, denom, emit)
    tree_forward(minus, numer + denom // 2, denom, emit)


def tree_inverse(size, numer, denom, load):
    if size == 1:
        return [load(numer, denom)]
    denom = 2 * denom
    cos, sin = math.cos(2 * math.pi * numer / denom), math.sin(2 * math.pi * numer / denom)
    plus = tree_inverse(size // 2, numer, denom, load)
    minus = tree_inverse(size // 2, numer + denom // 2, denom, load)
    low = [(a[0] + b[0], a[1] + b[1]) for a, b in zip(plus, minus)]
    high = []
    for a, b in zip(plus, minus):
        re, im = a[0] - b[0], a[1] - b[1]
        high.append((cos * re + sin * im, cos * im - sin * re))
    return low + high


def slot_of(numer, denom, devices):
    numer = (numer * (4 * devices // denom)) % (4 * devices)
    return (numer - 1) // 4


def spread_kernel(x_ref, out_far, out_ref, sems):
    devices = x_ref.shape[0]
    copies = []
    for op in range(FWD_OPS):
        values = [(x_ref[d, op], None) for d in range(devices)]

        def emit(numer, denom, value):
            slot = slot_of(numer, denom, devices)
            out_ref[op, slot, 0] = value[0]
            out_ref[op, slot, 1] = value[1]

        tree_forward(values, 1, 4, emit)
        copies.append(pltpu.make_async_copy(out_ref.at[op], out_far.at[:, op], sems.at[op]))
        copies[-1].start()
    for copy in copies:
        copy.wait()


def gather_kernel(u_ref, out_ref):
    devices = u_ref.shape[0]
    for out in range(2):

        def load(numer, denom):
            slot = slot_of(numer, denom, devices)
            return u_ref[slot, out, 0], u_ref[slot, out, 1]

        for block, pair in enumerate(tree_inverse(devices, 1, 4, load)):
            for k, value in enumerate(pair):
                index = k * devices + block
                out_ref[index // 2, out, index % 2] = value


def copy_all(pairs, sems):
    copies = [pltpu.make_async_copy(a, b, sems.at[k]) for k, (a, b) in enumerate(pairs)]
    for copy in copies:
        copy.start()
    return copies


def stack_kernel(*refs):
    operands, (out_far, near_ref, in_sems, out_sems) = refs[:-4], refs[-4:]
    copies = copy_all([(ref, near_ref.at[op]) for op, ref in enumerate(operands)], in_sems)
    leaving = []
    for op, copy in enumerate(copies):
        copy.wait()
        leaving += [pltpu.make_async_copy(near_ref.at[op], out_far.at[:, op], out_sems.at[op])]
        leaving[-1].start()
    for copy in leaving:
        copy.wait()


def deliver_kernel(in_ref, first_ref, second_ref, sems):
    pairs = [
        (in_ref.at[:, out, half], ref.at[half])
        for out, ref in enumerate((first_ref, second_ref))
        for half in range(2)
    ]
    for copy in copy_all(pairs, sems):
        copy.wait()


def spectrum_kernel(x_ref, a_ref, turn_ref, *rest, damp):
    totals_refs, rest = rest[:-10], rest[-10:]
    far, (out_ref, spec_ref, lhs_ref), near, sems = rest[:3], rest[3:6], rest[6:9], rest[9]
    b_ref, h_ref, ai_ref = near
    rows = turn_ref.shape[1]
    copies = copy_all(list(zip(far, near)), sems)

    def column_stage(table_ref, re, im):
        both = dot32(table_ref[...], tall_right(split16(jnp.concatenate([re, im], axis=1))))
        top, bottom = both[:rows], both[rows:]
        return top[:, :LANES] - bottom[:, LANES:], top[:, LANES:] + bottom[:, :LANES]

    for op in range(FWD_OPS):
        re, im = column_stage(
            a_ref, x_ref[:, op, 0].reshape(rows, LANES), x_ref[:, op, 1].reshape(rows, LANES)
        )
        turn_re, turn_im = turn_ref[0], turn_ref[1]
        turned = jnp.concatenate(
            [re * turn_re - im * turn_im, re * turn_im + im * turn_re], axis=1
        )
        lhs_ref[op] = wide_left(split16(turned))

    copies[0].wait()
    shape = spec_ref.shape
    left = lhs_ref[...].reshape(shape[0] * shape[1], lhs_ref.shape[2])
    spec_ref[...] = dot32(left, b_ref[0]).reshape(shape)
    for copy in copies[1:]:
        copy.wait()

    totals = sum(ref[...] for ref in totals_refs)
    totals = damp * jnp.sum(totals, axis=1, keepdims=True)

    def member(op):
        return spec_ref[op, :, :LANES], spec_ref[op, :, LANES:]

    def products(pairs):
        re, im = 0.0, 0.0
        for left, right in pairs:
            left_re, left_im = member(left)
            right_re, right_im = member(right)
            re = re + (left_re * right_re - left_im * right_im)
            im = im + (left_re * right_im + left_im * right_re)
        return re, im

    for out, pairs in enumerate((((2, 1), (0, 3)), ((4, 1), (0, 5), (6, 3)))):
        re, im = products(pairs)
        re = re + sum(totals[a : a + 1] * totals[b : b + 1] for a, b in pairs)
        h_re, h_im = h_ref[0], h_ref[1]
        damped = jnp.concatenate([re * h_re - im * h_im, re * h_im + im * h_re], axis=1)
        both = dot32(wide_left(split16(damped)), b_ref[1])
        re, im = both[:, :LANES], both[:, LANES:]
        turn_re, turn_im = turn_ref[0], turn_ref[1]
        re, im = re * turn_re + im * turn_im, im * turn_re - re * turn_im
        re, im = column_stage(ai_ref, re, im)
        for which, value in enumerate((re, im)):
            piece = (out_ref.shape[0],) + out_ref.shape[3:]
            out_ref[:, out, which] = value.reshape(piece)


def call(kernel, name, out_shapes, *args, near, scratch=()):
    spaces = [VMEM if flag else pltpu.MemorySpace.HBM for flag in near]
    args = [pltpu.with_memory_space_constraint(v, space) for v, space in zip(args, spaces)]
    specs = [pl.BlockSpec(memory_space=space) for space in spaces]
    outs = [space(shape, jnp.float32) for shape, space in zip(out_shapes, spaces[len(args) :])]
    return pl.pallas_call(
        kernel,
        out_shape=outs,
        in_specs=specs[: len(args)],
        out_specs=specs[len(args) :],
        scratch_shapes=scratch,
        compiler_params=pltpu.CompilerParams(vmem_limit_bytes=24 << 20),
        name=name,
    )(*args)


def exchange(value):
    return lax.all_to_all(value, AXES, split_axis=0, concat_axis=0, tiled=True)


def lane_tables():
    index = np.arange(LANES)
    angle = 2.0 * np.pi * ((index[:, None] * index[None, :]) % LANES) / LANES
    cos, sin = np.cos(angle), np.sin(angle)
    forward = np.block([[cos, sin], [-sin, cos]]).astype(np.float32)
    backward = np.block([[cos, -sin], [sin, cos]]).astype(np.float32)
    parts = []
    for table in (forward, backward):
        high = table.astype(jnp.bfloat16)
        low = (table - high.astype(np.float32)).astype(jnp.bfloat16)
        parts.append(np.concatenate([high, high, low], axis=0))
    return jnp.asarray(np.stack(parts))


def tables(local_limbs, devices, scaling, rate):
    rows = local_limbs // LANES
    period = 4 * local_limbs * devices
    freq = 4 * device_position() + 1

    def grid(shape):
        return (lax.broadcasted_iota(jnp.int32, shape, 0), lax.broadcasted_iota(jnp.int32, shape, 1))

    q1, t1 = grid((rows, rows))
    step = period // rows
    cos, sin = turn(((t1 * q1) % rows) * step + LANES * t1 * freq, period)
    forward = wide_left(split_table(jnp.concatenate([cos, sin], axis=0)))
    t1, q1 = grid((rows, rows))
    cos, sin = turn(((t1 * q1) % rows) * step + LANES * t1 * freq, period)
    backward = wide_left(split_table(jnp.concatenate([cos, -sin], axis=0)))
    q1, t2 = grid((rows, LANES))
    between = jnp.stack(turn(t2 * (q1 * (period // local_limbs) + freq), period))
    numer = freq + 4 * devices * (q1 + rows * t2)
    numer = jnp.where(2 * numer > period, numer - period, numer)
    angle = numer.astype(jnp.float32) * (2.0 * math.pi / period)
    half = jnp.sin(0.5 * angle)
    damp = math.exp(-rate)
    den_re = -math.expm1(-rate) + (2.0 * damp) * half * half
    den_im = -damp * jnp.sin(angle)
    norm = scaling / (den_re * den_re + den_im * den_im)
    filt = jnp.stack([den_re * norm, -den_im * norm])
    return forward, between, filt, backward


def weighted_sums(stacked, rate):
    local_limbs = stacked.shape[0] * stacked.shape[2] * LANES
    shape = (stacked.shape[0], 1, stacked.shape[2], LANES)
    index = (
        lax.broadcasted_iota(jnp.int32, shape, 0) * shape[2]
        + lax.broadcasted_iota(jnp.int32, shape, 2)
    ) * LANES + lax.broadcasted_iota(jnp.int32, shape, 3)
    left = (local_limbs - 1 - index) + (device_count() - 1 - device_position()) * local_limbs
    return jnp.sum(stacked * jnp.exp(left.astype(jnp.float32) * -rate), axis=(0, 2))


def sum_over_lanes(sums):
    count = lax.axis_size("lane")
    step = 1
    while step < count:
        sums = sums + lax.ppermute(sums, "lane", [(d, d ^ step) for d in range(count)])
        step *= 2
    return sums


def group_parts(sums):
    count = lax.axis_size("grp")
    step = 1
    parts = [sums]
    while step < count:
        sums = sum(parts[1:], parts[0])
        span = min(4, count // step)
        parts = [sums] + [
            lax.ppermute(sums, "grp", [(d, d ^ (step * k)) for d in range(count)])
            for k in range(1, span)
        ]
        step *= span
    return parts


def local(*operands):
    devices = device_count()
    local_limbs = operands[0].shape[0]
    total = local_limbs * devices
    rate = 1.0 / (2 * local_limbs)
    scaling = 1.0 / (16.0 * math.sqrt(total) * math.sqrt(local_limbs))
    rows = local_limbs // LANES
    piece = rows // devices
    inside = piece % 8 == 0

    dma = pltpu.SemaphoreType.DMA
    far_ops = [v.reshape(devices, piece, LANES) for v in operands]
    (stacked,) = call(
        stack_kernel,
        "stack",
        [(devices, FWD_OPS, piece, LANES)],
        *far_ops,
        near=[False] * (FWD_OPS + 1),
        scratch=[
            pltpu.VMEM((FWD_OPS, devices, piece, LANES), jnp.float32),
            dma((FWD_OPS,)),
            dma((FWD_OPS,)),
        ],
    )
    received = exchange(stacked)
    sums = sum_over_lanes(weighted_sums(stacked, rate))
    received, sums = lax.optimization_barrier((received, sums))
    forward, between, filt, backward = tables(local_limbs, devices, scaling / total, rate)
    parts = group_parts(sums)
    near_consts = (forward, between, *parts)
    far_consts = (lane_tables(), filt, backward)

    (spread,) = call(
        spread_kernel,
        "spread",
        [(devices, FWD_OPS, 2, piece, LANES)],
        received,
        near=[True, False],
        scratch=[
            pltpu.VMEM((FWD_OPS, devices, 2, piece, LANES), jnp.float32),
            dma((FWD_OPS,)),
        ],
    )
    landed = exchange(spread)
    if not inside:
        landed = landed.transpose(1, 2, 0, 3, 4).reshape(1, FWD_OPS, 2, rows, LANES)
    (turned,) = call(
        functools.partial(spectrum_kernel, damp=math.exp(-rate)),
        "spectrum",
        [(devices, 2, 2, piece, LANES) if inside else (1, 2, 2, rows, LANES)],
        landed,
        *near_consts,
        *far_consts,
        near=[True] * (1 + len(near_consts)) + [False] * 3 + [True],
        scratch=[
            pltpu.VMEM((FWD_OPS, rows, 2 * LANES), jnp.float32),
            pltpu.VMEM((FWD_OPS, rows, 6 * LANES), jnp.bfloat16),
        ]
        + [pltpu.VMEM(v.shape, v.dtype) for v in far_consts]
        + [dma((3,))],
    )
    if not inside:
        turned = turned.reshape(2, 2, devices, piece, LANES).transpose(2, 0, 1, 3, 4)
    gathered = exchange(turned)
    (coeffs,) = call(
        gather_kernel, "gather", [(devices, 2, 2, piece, LANES)], gathered, near=[True] * 2
    )
    owned = exchange(coeffs)
    results = call(
        deliver_kernel,
        "deliver",
        [(2, devices, piece, LANES)] * 2,
        owned,
        near=[True, False, False],
        scratch=[dma((4,))],
    )
    return tuple(v.reshape(2 * local_limbs) for v in results)


def solution(mesh):
    return jax.shard_map(
        local,
        mesh=mesh,
        in_specs=(P(AXES),) * FWD_OPS,
        out_specs=(P(AXES), P(AXES)),
        check_vma=False,
    )
```

```python
import functools
import math

import jax
import jax.numpy as jnp
import numpy as np
from jax import lax
from jax.experimental import pallas as pl
from jax.experimental.pallas import tpu as pltpu
from jax.sharding import PartitionSpec as P

AXES = ("grp", "lane")
LANES = 128
FWD_OPS = 7
VMEM = pltpu.MemorySpace.VMEM


def device_count():
    return lax.axis_size("grp") * lax.axis_size("lane")


def device_position():
    return lax.axis_index("grp") * lax.axis_size("lane") + lax.axis_index("lane")


def turn(numer, denom):
    reduced = numer % denom
    reduced = jnp.where(2 * reduced > denom, reduced - denom, reduced)
    angle = reduced.astype(jnp.float32) * (2.0 * math.pi / denom)
    return jnp.cos(angle), jnp.sin(angle)


def split16(value):
    high = value.astype(jnp.bfloat16)
    return high, (value - high.astype(jnp.float32)).astype(jnp.bfloat16)


def split_table(value):
    high = lax.reduce_precision(value, 8, 7)
    return high.astype(jnp.bfloat16), (value - high).astype(jnp.bfloat16)


def wide_left(parts):
    return jnp.concatenate([parts[0], parts[1], parts[0]], axis=1)


def tall_right(parts):
    return jnp.concatenate([parts[0], parts[0], parts[1]], axis=0)


def dot32(left, right):
    return jnp.dot(left, right, preferred_element_type=jnp.float32)


def tree_forward(values, numer, denom, emit):
    if len(values) == 1:
        emit(numer, denom, values[0])
        return
    half = len(values) // 2
    numer, denom = numer, 2 * denom
    cos, sin = math.cos(2 * math.pi * numer / denom), math.sin(2 * math.pi * numer / denom)
    plus, minus = [], []
    for low, high in zip(values[:half], values[half:]):
        if low[1] is None:
            re, im = cos * high[0], sin * high[0]
            plus.append((low[0] + re, im))
            minus.append((low[0] - re, -im))
        else:
            re = cos * high[0] - sin * high[1]
            im = sin * high[0] + cos * high[1]
            plus.append((low[0] + re, low[1] + im))
            minus.append((low[0] - re, low[1] - im))
    tree_forward(plus, numer, denom, emit)
    tree_forward(minus, numer + denom // 2, denom, emit)


def tree_inverse(size, numer, denom, load):
    if size == 1:
        return [load(numer, denom)]
    denom = 2 * denom
    cos, sin = math.cos(2 * math.pi * numer / denom), math.sin(2 * math.pi * numer / denom)
    plus = tree_inverse(size // 2, numer, denom, load)
    minus = tree_inverse(size // 2, numer + denom // 2, denom, load)
    low = [(a[0] + b[0], a[1] + b[1]) for a, b in zip(plus, minus)]
    high = []
    for a, b in zip(plus, minus):
        re, im = a[0] - b[0], a[1] - b[1]
        high.append((cos * re + sin * im, cos * im - sin * re))
    return low + high


def slot_of(numer, denom, devices):
    numer = (numer * (4 * devices // denom)) % (4 * devices)
    return (numer - 1) // 4


def spread_kernel(x_ref, out_far, out_ref, sems):
    devices = x_ref.shape[0]
    copies = []
    for op in range(FWD_OPS):
        values = [(x_ref[d, op], None) for d in range(devices)]

        def emit(numer, denom, value):
            slot = slot_of(numer, denom, devices)
            out_ref[op, slot, 0] = value[0]
            out_ref[op, slot, 1] = value[1]

        tree_forward(values, 1, 4, emit)
        copies.append(pltpu.make_async_copy(out_ref.at[op], out_far.at[:, op], sems.at[op]))
        copies[-1].start()
    for copy in copies:
        copy.wait()


def gather_kernel(u_ref, out_ref):
    devices = u_ref.shape[0]
    for out in range(2):

        def load(numer, denom):
            slot = slot_of(numer, denom, devices)
            return u_ref[slot, out, 0], u_ref[slot, out, 1]

        for block, pair in enumerate(tree_inverse(devices, 1, 4, load)):
            for k, value in enumerate(pair):
                index = k * devices + block
                out_ref[index // 2, out, index % 2] = value


def copy_all(pairs, sems):
    copies = [pltpu.make_async_copy(a, b, sems.at[k]) for k, (a, b) in enumerate(pairs)]
    for copy in copies:
        copy.start()
    return copies


def stack_kernel(*refs):
    operands, out_ref, sems = refs[:-2], refs[-2], refs[-1]
    pairs = [(ref, out_ref.at[:, op]) for op, ref in enumerate(operands)]
    for copy in copy_all(pairs, sems):
        copy.wait()


def deliver_kernel(in_ref, first_ref, second_ref, sems):
    pairs = [
        (in_ref.at[:, out, half], ref.at[half])
        for out, ref in enumerate((first_ref, second_ref))
        for half in range(2)
    ]
    for copy in copy_all(pairs, sems):
        copy.wait()


def spectrum_kernel(x_ref, a_ref, turn_ref, *rest, damp):
    totals_refs, rest = rest[:-10], rest[-10:]
    far, (out_ref, spec_ref, lhs_ref), near, sems = rest[:3], rest[3:6], rest[6:9], rest[9]
    b_ref, h_ref, ai_ref = near
    rows = turn_ref.shape[1]
    copies = copy_all(list(zip(far, near)), sems)

    def column_stage(table_ref, re, im):
        both = dot32(table_ref[...], tall_right(split16(jnp.concatenate([re, im], axis=1))))
        top, bottom = both[:rows], both[rows:]
        return top[:, :LANES] - bottom[:, LANES:], top[:, LANES:] + bottom[:, :LANES]

    for op in range(FWD_OPS):
        re, im = column_stage(
            a_ref, x_ref[:, op, 0].reshape(rows, LANES), x_ref[:, op, 1].reshape(rows, LANES)
        )
        turn_re, turn_im = turn_ref[0], turn_ref[1]
        turned = jnp.concatenate(
            [re * turn_re - im * turn_im, re * turn_im + im * turn_re], axis=1
        )
        lhs_ref[op] = wide_left(split16(turned))

    copies[0].wait()
    shape = spec_ref.shape
    left = lhs_ref[...].reshape(shape[0] * shape[1], lhs_ref.shape[2])
    spec_ref[...] = dot32(left, b_ref[0]).reshape(shape)
    for copy in copies[1:]:
        copy.wait()

    totals = sum(ref[...] for ref in totals_refs)
    totals = damp * jnp.sum(totals, axis=1, keepdims=True)

    def member(op):
        return spec_ref[op, :, :LANES], spec_ref[op, :, LANES:]

    def products(pairs):
        re, im = 0.0, 0.0
        for left, right in pairs:
            left_re, left_im = member(left)
            right_re, right_im = member(right)
            re = re + (left_re * right_re - left_im * right_im)
            im = im + (left_re * right_im + left_im * right_re)
        return re, im

    for out, pairs in enumerate((((2, 1), (0, 3)), ((4, 1), (0, 5), (6, 3)))):
        re, im = products(pairs)
        re = re + sum(totals[a : a + 1] * totals[b : b + 1] for a, b in pairs)
        h_re, h_im = h_ref[0], h_ref[1]
        damped = jnp.concatenate([re * h_re - im * h_im, re * h_im + im * h_re], axis=1)
        both = dot32(wide_left(split16(damped)), b_ref[1])
        re, im = both[:, :LANES], both[:, LANES:]
        turn_re, turn_im = turn_ref[0], turn_ref[1]
        re, im = re * turn_re + im * turn_im, im * turn_re - re * turn_im
        re, im = column_stage(ai_ref, re, im)
        for which, value in enumerate((re, im)):
            piece = (out_ref.shape[0],) + out_ref.shape[3:]
            out_ref[:, out, which] = value.reshape(piece)


def call(kernel, name, out_shapes, *args, near, scratch=()):
    spaces = [VMEM if flag else pltpu.MemorySpace.HBM for flag in near]
    args = [pltpu.with_memory_space_constraint(v, space) for v, space in zip(args, spaces)]
    specs = [pl.BlockSpec(memory_space=space) for space in spaces]
    outs = [space(shape, jnp.float32) for shape, space in zip(out_shapes, spaces[len(args) :])]
    return pl.pallas_call(
        kernel,
        out_shape=outs,
        in_specs=specs[: len(args)],
        out_specs=specs[len(args) :],
        scratch_shapes=scratch,
        compiler_params=pltpu.CompilerParams(vmem_limit_bytes=24 << 20),
        name=name,
    )(*args)


def exchange(value):
    return lax.all_to_all(value, AXES, split_axis=0, concat_axis=0, tiled=True)


def lane_tables():
    index = np.arange(LANES)
    angle = 2.0 * np.pi * ((index[:, None] * index[None, :]) % LANES) / LANES
    cos, sin = np.cos(angle), np.sin(angle)
    forward = np.block([[cos, sin], [-sin, cos]]).astype(np.float32)
    backward = np.block([[cos, -sin], [sin, cos]]).astype(np.float32)
    parts = []
    for table in (forward, backward):
        high = table.astype(jnp.bfloat16)
        low = (table - high.astype(np.float32)).astype(jnp.bfloat16)
        parts.append(np.concatenate([high, high, low], axis=0))
    return jnp.asarray(np.stack(parts))


def tables(local_limbs, devices, scaling, rate):
    rows = local_limbs // LANES
    period = 4 * local_limbs * devices
    freq = 4 * device_position() + 1

    def grid(shape):
        return (lax.broadcasted_iota(jnp.int32, shape, 0), lax.broadcasted_iota(jnp.int32, shape, 1))

    q1, t1 = grid((rows, rows))
    step = period // rows
    cos, sin = turn(((t1 * q1) % rows) * step + LANES * t1 * freq, period)
    forward = wide_left(split_table(jnp.concatenate([cos, sin], axis=0)))
    t1, q1 = grid((rows, rows))
    cos, sin = turn(((t1 * q1) % rows) * step + LANES * t1 * freq, period)
    backward = wide_left(split_table(jnp.concatenate([cos, -sin], axis=0)))
    q1, t2 = grid((rows, LANES))
    between = jnp.stack(turn(t2 * (q1 * (period // local_limbs) + freq), period))
    numer = freq + 4 * devices * (q1 + rows * t2)
    numer = jnp.where(2 * numer > period, numer - period, numer)
    angle = numer.astype(jnp.float32) * (2.0 * math.pi / period)
    half = jnp.sin(0.5 * angle)
    damp = math.exp(-rate)
    den_re = -math.expm1(-rate) + (2.0 * damp) * half * half
    den_im = -damp * jnp.sin(angle)
    norm = scaling / (den_re * den_re + den_im * den_im)
    filt = jnp.stack([den_re * norm, -den_im * norm])
    return forward, between, filt, backward


def weighted_sums(received, rate):
    devices, _, piece, _ = received.shape
    shape = (devices, 1, piece, LANES)
    index = lax.broadcasted_iota(jnp.int32, shape, 2) + device_position() * piece
    index = index + lax.broadcasted_iota(jnp.int32, shape, 0) * (devices * piece)
    index = index * LANES + lax.broadcasted_iota(jnp.int32, shape, 3)
    left = devices * devices * piece * LANES - 1 - index
    return jnp.sum(received * jnp.exp(left.astype(jnp.float32) * -rate), axis=(0, 2))


def sum_over_lanes(sums):
    count = lax.axis_size("lane")
    step = 1
    while step < count:
        sums = sums + lax.ppermute(sums, "lane", [(d, d ^ step) for d in range(count)])
        step *= 2
    return sums


def group_parts(sums):
    count = lax.axis_size("grp")
    step = 1
    parts = [sums]
    while step < count:
        sums = sum(parts[1:], parts[0])
        span = min(4, count // step)
        parts = [sums] + [
            lax.ppermute(sums, "grp", [(d, d ^ (step * k)) for d in range(count)])
            for k in range(1, span)
        ]
        step *= span
    return parts


def local(*operands):
    devices = device_count()
    local_limbs = operands[0].shape[0]
    total = local_limbs * devices
    rate = 1.0 / (2 * local_limbs)
    scaling = 1.0 / (16.0 * math.sqrt(total) * math.sqrt(local_limbs))
    rows = local_limbs // LANES
    piece = rows // devices
    inside = piece % 8 == 0

    dma = pltpu.SemaphoreType.DMA
    far_ops = [v.reshape(devices, piece, LANES) for v in operands]
    (stacked,) = call(
        stack_kernel,
        "stack",
        [(devices, FWD_OPS, piece, LANES)],
        *far_ops,
        near=[False] * FWD_OPS + [True],
        scratch=[dma((FWD_OPS,))],
    )
    received = exchange(stacked)
    sums = sum_over_lanes(weighted_sums(received, rate))
    forward, between, filt, backward = tables(local_limbs, devices, scaling / total, rate)
    parts = group_parts(sums)
    near_consts = (forward, between, *parts)
    far_consts = (lane_tables(), filt, backward)

    (spread,) = call(
        spread_kernel,
        "spread",
        [(devices, FWD_OPS, 2, piece, LANES)],
        received,
        near=[True, False],
        scratch=[
            pltpu.VMEM((FWD_OPS, devices, 2, piece, LANES), jnp.float32),
            dma((FWD_OPS,)),
        ],
    )
    landed = exchange(spread)
    if not inside:
        landed = landed.transpose(1, 2, 0, 3, 4).reshape(1, FWD_OPS, 2, rows, LANES)
    (turned,) = call(
        functools.partial(spectrum_kernel, damp=math.exp(-rate)),
        "spectrum",
        [(devices, 2, 2, piece, LANES) if inside else (1, 2, 2, rows, LANES)],
        landed,
        *near_consts,
        *far_consts,
        near=[True] * (1 + len(near_consts)) + [False] * 3 + [True],
        scratch=[
            pltpu.VMEM((FWD_OPS, rows, 2 * LANES), jnp.float32),
            pltpu.VMEM((FWD_OPS, rows, 6 * LANES), jnp.bfloat16),
        ]
        + [pltpu.VMEM(v.shape, v.dtype) for v in far_consts]
        + [dma((3,))],
    )
    if not inside:
        turned = turned.reshape(2, 2, devices, piece, LANES).transpose(2, 0, 1, 3, 4)
    gathered = exchange(turned)
    (coeffs,) = call(
        gather_kernel, "gather", [(devices, 2, 2, piece, LANES)], gathered, near=[True] * 2
    )
    owned = exchange(coeffs)
    results = call(
        deliver_kernel,
        "deliver",
        [(2, devices, piece, LANES)] * 2,
        owned,
        near=[True, False, False],
        scratch=[dma((4,))],
    )
    return tuple(v.reshape(2 * local_limbs) for v in results)


def solution(mesh):
    return jax.shard_map(
        local,
        mesh=mesh,
        in_specs=(P(AXES),) * FWD_OPS,
        out_specs=(P(AXES), P(AXES)),
        check_vma=False,
    )
```

```python
import functools
import math

import jax
import jax.numpy as jnp
import numpy as np
from jax import lax
from jax.experimental import pallas as pl
from jax.experimental.pallas import tpu as pltpu
from jax.sharding import PartitionSpec as P

AXES = ("grp", "lane")
LANES = 128
FWD_OPS = 7
VMEM = pltpu.MemorySpace.VMEM


def device_count():
    return lax.axis_size("grp") * lax.axis_size("lane")


def device_position():
    return lax.axis_index("grp") * lax.axis_size("lane") + lax.axis_index("lane")


def turn(numer, denom):
    reduced = numer % denom
    reduced = jnp.where(2 * reduced > denom, reduced - denom, reduced)
    angle = reduced.astype(jnp.float32) * (2.0 * math.pi / denom)
    return jnp.cos(angle), jnp.sin(angle)


def split16(value):
    high = value.astype(jnp.bfloat16)
    return high, (value - high.astype(jnp.float32)).astype(jnp.bfloat16)


def split_table(value):
    high = lax.reduce_precision(value, 8, 7)
    return high.astype(jnp.bfloat16), (value - high).astype(jnp.bfloat16)


def wide_left(parts):
    return jnp.concatenate([parts[0], parts[1], parts[0]], axis=1)


def tall_right(parts):
    return jnp.concatenate([parts[0], parts[0], parts[1]], axis=0)


def dot32(left, right):
    return jnp.dot(left, right, preferred_element_type=jnp.float32)


def tree_forward(values, numer, denom, emit):
    if len(values) == 1:
        emit(numer, denom, values[0])
        return
    half = len(values) // 2
    numer, denom = numer, 2 * denom
    cos, sin = math.cos(2 * math.pi * numer / denom), math.sin(2 * math.pi * numer / denom)
    plus, minus = [], []
    for low, high in zip(values[:half], values[half:]):
        if low[1] is None:
            re, im = cos * high[0], sin * high[0]
            plus.append((low[0] + re, im))
            minus.append((low[0] - re, -im))
        else:
            re = cos * high[0] - sin * high[1]
            im = sin * high[0] + cos * high[1]
            plus.append((low[0] + re, low[1] + im))
            minus.append((low[0] - re, low[1] - im))
    tree_forward(plus, numer, denom, emit)
    tree_forward(minus, numer + denom // 2, denom, emit)


def tree_inverse(size, numer, denom, load):
    if size == 1:
        return [load(numer, denom)]
    denom = 2 * denom
    cos, sin = math.cos(2 * math.pi * numer / denom), math.sin(2 * math.pi * numer / denom)
    plus = tree_inverse(size // 2, numer, denom, load)
    minus = tree_inverse(size // 2, numer + denom // 2, denom, load)
    low = [(a[0] + b[0], a[1] + b[1]) for a, b in zip(plus, minus)]
    high = []
    for a, b in zip(plus, minus):
        re, im = a[0] - b[0], a[1] - b[1]
        high.append((cos * re + sin * im, cos * im - sin * re))
    return low + high


def slot_of(numer, denom, devices):
    numer = (numer * (4 * devices // denom)) % (4 * devices)
    return (numer - 1) // 4


def spread_kernel(x_ref, out_far, out_ref, sems):
    devices = x_ref.shape[0]
    copies = []
    for op in range(FWD_OPS):
        values = [(x_ref[d, op], None) for d in range(devices)]

        def emit(numer, denom, value):
            slot = slot_of(numer, denom, devices)
            out_ref[op, slot, 0] = value[0]
            out_ref[op, slot, 1] = value[1]

        tree_forward(values, 1, 4, emit)
        copies.append(pltpu.make_async_copy(out_ref.at[op], out_far.at[:, op], sems.at[op]))
        copies[-1].start()
    for copy in copies:
        copy.wait()


def gather_kernel(u_ref, out_ref):
    devices = u_ref.shape[0]
    for out in range(2):

        def load(numer, denom):
            slot = slot_of(numer, denom, devices)
            return u_ref[slot, out, 0], u_ref[slot, out, 1]

        for block, pair in enumerate(tree_inverse(devices, 1, 4, load)):
            for k, value in enumerate(pair):
                index = k * devices + block
                out_ref[index // 2, out, index % 2] = value


def copy_all(pairs, sems):
    copies = [pltpu.make_async_copy(a, b, sems.at[k]) for k, (a, b) in enumerate(pairs)]
    for copy in copies:
        copy.start()
    return copies


def stack_kernel(*refs):
    operands, out_ref, sems = refs[:-2], refs[-2], refs[-1]
    pairs = [(ref, out_ref.at[:, op]) for op, ref in enumerate(operands)]
    for copy in copy_all(pairs, sems):
        copy.wait()


def deliver_kernel(in_ref, first_ref, second_ref, sems):
    pairs = [
        (in_ref.at[:, out, half], ref.at[half])
        for out, ref in enumerate((first_ref, second_ref))
        for half in range(2)
    ]
    for copy in copy_all(pairs, sems):
        copy.wait()


def spectrum_kernel(x_ref, a_ref, ai_ref, turn_ref, h_ref, roots_ref, *rest, damp):
    totals_refs, (b_far, out_ref, spec_ref, lhs_ref, b_ref, sems) = rest[:-6], rest[-6:]
    rows = turn_ref.shape[1]
    copies = copy_all([(b_far, b_ref)], sems)

    quarter = rows // 4
    rho = (roots_ref[0:1], roots_ref[1:2])
    sigma = (roots_ref[2:3], roots_ref[3:4])

    def times(a, b):
        return a[0] * b[0] - a[1] * b[1], a[0] * b[1] + a[1] * b[0]

    def times_conj(a, b):
        return a[0] * b[0] + a[1] * b[1], a[1] * b[0] - a[0] * b[1]

    def add(a, b):
        return a[0] + b[0], a[1] + b[1]

    def sub(a, b):
        return a[0] - b[0], a[1] - b[1]

    def section(table, value):
        high, low = split16(jnp.concatenate(value, axis=1))
        both = dot32(table, jnp.concatenate([high, low, high, low], axis=0))
        top, bottom = both[:quarter], both[quarter:]
        return top[:, :LANES] - bottom[:, LANES:], top[:, LANES:] + bottom[:, :LANES]

    def join(values):
        return tuple(jnp.concatenate([v[k] for v in values], axis=0) for k in range(2))

    def cut(re, im):
        parts = [slice(m * quarter, (m + 1) * quarter) for m in range(4)]
        return [(re[part], im[part]) for part in parts]

    def column_forward(re, im):
        x = cut(re, im)
        turned = [times(x[2], rho), times(x[3], rho)]
        plus = [add(x[0], turned[0]), add(x[1], turned[1])]
        minus = [sub(x[0], turned[0]), sub(x[1], turned[1])]
        even, odd = times(plus[1], sigma), times(minus[1], sigma)
        odd = (-odd[1], odd[0])
        nodes = [add(plus[0], even), add(minus[0], odd), sub(plus[0], even), sub(minus[0], odd)]
        return join([section(a_ref[j], nodes[j]) for j in range(4)])

    def column_inverse(re, im):
        nodes = [section(ai_ref[j], value) for j, value in enumerate(cut(re, im))]
        odd = sub(nodes[1], nodes[3])
        plus = [add(nodes[0], nodes[2]), times_conj(sub(nodes[0], nodes[2]), sigma)]
        minus = [add(nodes[1], nodes[3]), times_conj((odd[1], -odd[0]), sigma)]
        low = [add(plus[m], minus[m]) for m in range(2)]
        high = [times_conj(sub(plus[m], minus[m]), rho) for m in range(2)]
        return join(low + high)

    for op in range(FWD_OPS):
        re, im = column_forward(
            x_ref[:, op, 0].reshape(rows, LANES), x_ref[:, op, 1].reshape(rows, LANES)
        )
        turn_re, turn_im = turn_ref[0], turn_ref[1]
        turned = jnp.concatenate(
            [re * turn_re - im * turn_im, re * turn_im + im * turn_re], axis=1
        )
        lhs_ref[op] = wide_left(split16(turned))

    copies[0].wait()
    shape = spec_ref.shape
    left = lhs_ref[...].reshape(shape[0] * shape[1], lhs_ref.shape[2])
    spec_ref[...] = dot32(left, b_ref[0]).reshape(shape)

    totals = sum(ref[...] for ref in totals_refs)
    totals = damp * jnp.sum(totals, axis=1, keepdims=True)

    def member(op):
        return spec_ref[op, :, :LANES], spec_ref[op, :, LANES:]

    def products(pairs):
        re, im = 0.0, 0.0
        for left, right in pairs:
            left_re, left_im = member(left)
            right_re, right_im = member(right)
            re = re + (left_re * right_re - left_im * right_im)
            im = im + (left_re * right_im + left_im * right_re)
        return re, im

    for out, pairs in enumerate((((2, 1), (0, 3)), ((4, 1), (0, 5), (6, 3)))):
        re, im = products(pairs)
        re = re + sum(totals[a : a + 1] * totals[b : b + 1] for a, b in pairs)
        h_re, h_im = h_ref[0], h_ref[1]
        damped = jnp.concatenate([re * h_re - im * h_im, re * h_im + im * h_re], axis=1)
        both = dot32(wide_left(split16(damped)), b_ref[1])
        re, im = both[:, :LANES], both[:, LANES:]
        turn_re, turn_im = turn_ref[0], turn_ref[1]
        re, im = re * turn_re + im * turn_im, im * turn_re - re * turn_im
        re, im = column_inverse(re, im)
        for which, value in enumerate((re, im)):
            piece = (out_ref.shape[0],) + out_ref.shape[3:]
            out_ref[:, out, which] = value.reshape(piece)


def call(kernel, name, out_shapes, *args, near, scratch=()):
    spaces = [VMEM if flag else pltpu.MemorySpace.HBM for flag in near]
    args = [pltpu.with_memory_space_constraint(v, space) for v, space in zip(args, spaces)]
    specs = [pl.BlockSpec(memory_space=space) for space in spaces]
    outs = [space(shape, jnp.float32) for shape, space in zip(out_shapes, spaces[len(args) :])]
    return pl.pallas_call(
        kernel,
        out_shape=outs,
        in_specs=specs[: len(args)],
        out_specs=specs[len(args) :],
        scratch_shapes=scratch,
        compiler_params=pltpu.CompilerParams(vmem_limit_bytes=24 << 20),
        name=name,
    )(*args)


def exchange(value):
    return lax.all_to_all(value, AXES, split_axis=0, concat_axis=0, tiled=True)


def lane_tables():
    index = np.arange(LANES)
    angle = 2.0 * np.pi * ((index[:, None] * index[None, :]) % LANES) / LANES
    cos, sin = np.cos(angle), np.sin(angle)
    forward = np.block([[cos, sin], [-sin, cos]]).astype(np.float32)
    backward = np.block([[cos, -sin], [sin, cos]]).astype(np.float32)
    parts = []
    for table in (forward, backward):
        high = table.astype(jnp.bfloat16)
        low = (table - high.astype(np.float32)).astype(jnp.bfloat16)
        parts.append(np.concatenate([high, high, low], axis=0))
    return jnp.asarray(np.stack(parts))


def tables(local_limbs, devices, scaling, rate):
    rows = local_limbs // LANES
    period = 4 * local_limbs * devices
    freq = 4 * device_position() + 1

    def grid(shape):
        return (lax.broadcasted_iota(jnp.int32, shape, 0), lax.broadcasted_iota(jnp.int32, shape, 1))

    quarter = rows // 4

    def section(conjugate):
        shape = (4, quarter, quarter)
        node = lax.broadcasted_iota(jnp.int32, shape, 0)
        k = lax.broadcasted_iota(jnp.int32, shape, 2 if conjugate else 1)
        t1 = lax.broadcasted_iota(jnp.int32, shape, 1 if conjugate else 2)
        cos, sin = turn(t1 * (freq + 4 * devices * (4 * k + node)) * LANES, period)
        table = jnp.concatenate([cos, -sin if conjugate else sin], axis=1)
        high, low = split_table(table)
        return jnp.concatenate([high, high, low, low], axis=2)

    forward, backward = section(False), section(True)
    row, t2 = grid((rows, LANES))
    q1 = 4 * (row % quarter) + row // quarter
    between = jnp.stack(turn(t2 * (q1 * (period // local_limbs) + freq), period))
    spread_freq = freq + lax.broadcasted_iota(jnp.int32, (LANES,), 0) * 0
    roots = jnp.stack(turn(spread_freq, 8 * devices) + turn(spread_freq, 16 * devices))
    numer = freq + 4 * devices * (q1 + rows * t2)
    numer = jnp.where(2 * numer > period, numer - period, numer)
    angle = numer.astype(jnp.float32) * (2.0 * math.pi / period)
    half = jnp.sin(0.5 * angle)
    damp = math.exp(-rate)
    den_re = -math.expm1(-rate) + (2.0 * damp) * half * half
    den_im = -damp * jnp.sin(angle)
    norm = scaling / (den_re * den_re + den_im * den_im)
    filt = jnp.stack([den_re * norm, -den_im * norm])
    return forward, backward, between, filt, roots


def weighted_sums(received, rate):
    devices, _, piece, _ = received.shape
    shape = (devices, 1, piece, LANES)
    index = lax.broadcasted_iota(jnp.int32, shape, 2) + device_position() * piece
    index = index + lax.broadcasted_iota(jnp.int32, shape, 0) * (devices * piece)
    index = index * LANES + lax.broadcasted_iota(jnp.int32, shape, 3)
    left = devices * devices * piece * LANES - 1 - index
    return jnp.sum(received * jnp.exp(left.astype(jnp.float32) * -rate), axis=(0, 2))


def sum_over_lanes(sums):
    count = lax.axis_size("lane")
    step = 1
    while step < count:
        sums = sums + lax.ppermute(sums, "lane", [(d, d ^ step) for d in range(count)])
        step *= 2
    return sums


def group_parts(sums):
    count = lax.axis_size("grp")
    step = 1
    parts = [sums]
    while step < count:
        sums = sum(parts[1:], parts[0])
        span = min(4, count // step)
        parts = [sums] + [
            lax.ppermute(sums, "grp", [(d, d ^ (step * k)) for d in range(count)])
            for k in range(1, span)
        ]
        step *= span
    return parts


def local(*operands):
    devices = device_count()
    local_limbs = operands[0].shape[0]
    total = local_limbs * devices
    rate = 1.0 / (2 * local_limbs)
    scaling = 1.0 / (16.0 * math.sqrt(total) * math.sqrt(local_limbs))
    rows = local_limbs // LANES
    piece = rows // devices
    inside = piece % 8 == 0

    dma = pltpu.SemaphoreType.DMA
    far_ops = [v.reshape(devices, piece, LANES) for v in operands]
    (stacked,) = call(
        stack_kernel,
        "stack",
        [(devices, FWD_OPS, piece, LANES)],
        *far_ops,
        near=[False] * FWD_OPS + [True],
        scratch=[dma((FWD_OPS,))],
    )
    received = exchange(stacked)
    sums = sum_over_lanes(weighted_sums(received, rate))
    near_tables = tables(local_limbs, devices, scaling / total, rate)
    parts = group_parts(sums)
    near_consts = (*near_tables, *parts)
    lane_table = lane_tables()

    (spread,) = call(
        spread_kernel,
        "spread",
        [(devices, FWD_OPS, 2, piece, LANES)],
        received,
        near=[True, False],
        scratch=[
            pltpu.VMEM((FWD_OPS, devices, 2, piece, LANES), jnp.float32),
            dma((FWD_OPS,)),
        ],
    )
    landed = exchange(spread)
    if not inside:
        landed = landed.transpose(1, 2, 0, 3, 4).reshape(1, FWD_OPS, 2, rows, LANES)
    (turned,) = call(
        functools.partial(spectrum_kernel, damp=math.exp(-rate)),
        "spectrum",
        [(devices, 2, 2, piece, LANES) if inside else (1, 2, 2, rows, LANES)],
        landed,
        *near_consts,
        lane_table,
        near=[True] * (1 + len(near_consts)) + [False, True],
        scratch=[
            pltpu.VMEM((FWD_OPS, rows, 2 * LANES), jnp.float32),
            pltpu.VMEM((FWD_OPS, rows, 6 * LANES), jnp.bfloat16),
            pltpu.VMEM(lane_table.shape, lane_table.dtype),
            dma((1,)),
        ],
    )
    if not inside:
        turned = turned.reshape(2, 2, devices, piece, LANES).transpose(2, 0, 1, 3, 4)
    gathered = exchange(turned)
    (coeffs,) = call(
        gather_kernel, "gather", [(devices, 2, 2, piece, LANES)], gathered, near=[True] * 2
    )
    owned = exchange(coeffs)
    results = call(
        deliver_kernel,
        "deliver",
        [(2, devices, piece, LANES)] * 2,
        owned,
        near=[True, False, False],
        scratch=[dma((4,))],
    )
    return tuple(v.reshape(2 * local_limbs) for v in results)


def solution(mesh):
    return jax.shard_map(
        local,
        mesh=mesh,
        in_specs=(P(AXES),) * FWD_OPS,
        out_specs=(P(AXES), P(AXES)),
        check_vma=False,
    )
```

```python
import functools
import math

import jax
import jax.numpy as jnp
import numpy as np
from jax import lax
from jax.experimental import pallas as pl
from jax.experimental.pallas import tpu as pltpu
from jax.sharding import PartitionSpec as P

AXES = ("grp", "lane")
LANES = 128
FWD_OPS = 7
VMEM = pltpu.MemorySpace.VMEM


def device_count():
    return lax.axis_size("grp") * lax.axis_size("lane")


def device_position():
    return lax.axis_index("grp") * lax.axis_size("lane") + lax.axis_index("lane")


def turn(numer, denom):
    reduced = numer % denom
    reduced = jnp.where(2 * reduced > denom, reduced - denom, reduced)
    angle = reduced.astype(jnp.float32) * (2.0 * math.pi / denom)
    return jnp.cos(angle), jnp.sin(angle)


def split16(value):
    high = value.astype(jnp.bfloat16)
    return high, (value - high.astype(jnp.float32)).astype(jnp.bfloat16)


def split_table(value):
    high = lax.reduce_precision(value, 8, 7)
    return high.astype(jnp.bfloat16), (value - high).astype(jnp.bfloat16)


def wide_left(parts):
    return jnp.concatenate([parts[0], parts[1], parts[0]], axis=1)


def tall_right(parts):
    return jnp.concatenate([parts[0], parts[0], parts[1]], axis=0)


def dot32(left, right):
    return jnp.dot(left, right, preferred_element_type=jnp.float32)


def tree_forward(values, numer, denom, emit):
    if len(values) == 1:
        emit(numer, denom, values[0])
        return
    half = len(values) // 2
    numer, denom = numer, 2 * denom
    cos, sin = math.cos(2 * math.pi * numer / denom), math.sin(2 * math.pi * numer / denom)
    plus, minus = [], []
    for low, high in zip(values[:half], values[half:]):
        if low[1] is None:
            re, im = cos * high[0], sin * high[0]
            plus.append((low[0] + re, im))
            minus.append((low[0] - re, -im))
        else:
            re = cos * high[0] - sin * high[1]
            im = sin * high[0] + cos * high[1]
            plus.append((low[0] + re, low[1] + im))
            minus.append((low[0] - re, low[1] - im))
    tree_forward(plus, numer, denom, emit)
    tree_forward(minus, numer + denom // 2, denom, emit)


def tree_inverse(size, numer, denom, load):
    if size == 1:
        return [load(numer, denom)]
    denom = 2 * denom
    cos, sin = math.cos(2 * math.pi * numer / denom), math.sin(2 * math.pi * numer / denom)
    plus = tree_inverse(size // 2, numer, denom, load)
    minus = tree_inverse(size // 2, numer + denom // 2, denom, load)
    low = [(a[0] + b[0], a[1] + b[1]) for a, b in zip(plus, minus)]
    high = []
    for a, b in zip(plus, minus):
        re, im = a[0] - b[0], a[1] - b[1]
        high.append((cos * re + sin * im, cos * im - sin * re))
    return low + high


def slot_of(numer, denom, devices):
    numer = (numer * (4 * devices // denom)) % (4 * devices)
    return (numer - 1) // 4


def spread_kernel(x_ref, out_far, out_ref, sems):
    devices = x_ref.shape[0]
    copies = []
    for op in range(FWD_OPS):
        values = [(x_ref[d, op], None) for d in range(devices)]

        def emit(numer, denom, value):
            slot = slot_of(numer, denom, devices)
            out_ref[op, slot, 0] = value[0]
            out_ref[op, slot, 1] = value[1]

        tree_forward(values, 1, 4, emit)
        copies.append(pltpu.make_async_copy(out_ref.at[op], out_far.at[:, op], sems.at[op]))
        copies[-1].start()
    for copy in copies:
        copy.wait()


def gather_kernel(u_ref, out_ref):
    devices = u_ref.shape[0]
    for out in range(2):

        def load(numer, denom):
            slot = slot_of(numer, denom, devices)
            return u_ref[slot, out, 0], u_ref[slot, out, 1]

        for block, pair in enumerate(tree_inverse(devices, 1, 4, load)):
            for k, value in enumerate(pair):
                index = k * devices + block
                out_ref[index // 2, out, index % 2] = value


def copy_all(pairs, sems):
    copies = [pltpu.make_async_copy(a, b, sems.at[k]) for k, (a, b) in enumerate(pairs)]
    for copy in copies:
        copy.start()
    return copies


def stack_kernel(*refs):
    operands, out_ref, sems = refs[:-2], refs[-2], refs[-1]
    pairs = [(ref, out_ref.at[:, op]) for op, ref in enumerate(operands)]
    for copy in copy_all(pairs, sems):
        copy.wait()


def deliver_kernel(in_ref, first_ref, second_ref, sems):
    pairs = [
        (in_ref.at[:, out, half], ref.at[half])
        for out, ref in enumerate((first_ref, second_ref))
        for half in range(2)
    ]
    for copy in copy_all(pairs, sems):
        copy.wait()


def spectrum_kernel(x_ref, a_ref, ai_ref, turn_ref, h_ref, roots_ref, *rest, damp):
    totals_refs, (b_far, out_ref, spec_ref, lhs_ref, b_ref, sems) = rest[:-6], rest[-6:]
    rows = turn_ref.shape[1]
    copies = copy_all([(b_far, b_ref)], sems)

    quarter = rows // 4
    rho = (roots_ref[0:1], roots_ref[1:2])
    sigma = (roots_ref[2:3], roots_ref[3:4])

    def times(a, b):
        return a[0] * b[0] - a[1] * b[1], a[0] * b[1] + a[1] * b[0]

    def times_conj(a, b):
        return a[0] * b[0] + a[1] * b[1], a[1] * b[0] - a[0] * b[1]

    def add(a, b):
        return a[0] + b[0], a[1] + b[1]

    def sub(a, b):
        return a[0] - b[0], a[1] - b[1]

    def section(table, value):
        high, low = split16(jnp.concatenate(value, axis=1))
        both = dot32(table, jnp.concatenate([high, low, high, low], axis=0))
        top, bottom = both[:quarter], both[quarter:]
        return top[:, :LANES] - bottom[:, LANES:], top[:, LANES:] + bottom[:, :LANES]

    def join(values):
        return tuple(jnp.concatenate([v[k] for v in values], axis=0) for k in range(2))

    def cut(re, im):
        parts = [slice(m * quarter, (m + 1) * quarter) for m in range(4)]
        return [(re[part], im[part]) for part in parts]

    def column_forward(re, im):
        x = cut(re, im)
        turned = [times(x[2], rho), times(x[3], rho)]
        plus = [add(x[0], turned[0]), add(x[1], turned[1])]
        minus = [sub(x[0], turned[0]), sub(x[1], turned[1])]
        even, odd = times(plus[1], sigma), times(minus[1], sigma)
        odd = (-odd[1], odd[0])
        nodes = [add(plus[0], even), add(minus[0], odd), sub(plus[0], even), sub(minus[0], odd)]
        return join([section(a_ref[j], nodes[j]) for j in range(4)])

    def column_inverse(re, im):
        nodes = [section(ai_ref[j], value) for j, value in enumerate(cut(re, im))]
        odd = sub(nodes[1], nodes[3])
        plus = [add(nodes[0], nodes[2]), times_conj(sub(nodes[0], nodes[2]), sigma)]
        minus = [add(nodes[1], nodes[3]), times_conj((odd[1], -odd[0]), sigma)]
        low = [add(plus[m], minus[m]) for m in range(2)]
        high = [times_conj(sub(plus[m], minus[m]), rho) for m in range(2)]
        return join(low + high)

    def forward(first, last):
        for op in range(first, last):
            re, im = column_forward(
                x_ref[:, op, 0].reshape(rows, LANES), x_ref[:, op, 1].reshape(rows, LANES)
            )
            turn_re, turn_im = turn_ref[0], turn_ref[1]
            turned = jnp.concatenate(
                [re * turn_re - im * turn_im, re * turn_im + im * turn_re], axis=1
            )
            lhs_ref[op] = wide_left(split16(turned))
        if first == 0:
            copies[0].wait()
        count = last - first
        left = lhs_ref[first:last].reshape(count * rows, lhs_ref.shape[2])
        spec_ref[first:last] = dot32(left, b_ref[0]).reshape(count, rows, 2 * LANES)

    forward(0, 4)
    forward(4, FWD_OPS)

    totals = sum(ref[...] for ref in totals_refs)
    totals = damp * jnp.sum(totals, axis=1, keepdims=True)

    def member(op):
        return spec_ref[op, :, :LANES], spec_ref[op, :, LANES:]

    def products(pairs):
        re, im = 0.0, 0.0
        for left, right in pairs:
            left_re, left_im = member(left)
            right_re, right_im = member(right)
            re = re + (left_re * right_re - left_im * right_im)
            im = im + (left_re * right_im + left_im * right_re)
        return re, im

    def backward(out, pairs):
        re, im = products(pairs)
        re = re + sum(totals[a : a + 1] * totals[b : b + 1] for a, b in pairs)
        h_re, h_im = h_ref[0], h_ref[1]
        damped = jnp.concatenate([re * h_re - im * h_im, re * h_im + im * h_re], axis=1)
        both = dot32(wide_left(split16(damped)), b_ref[1])
        re, im = both[:, :LANES], both[:, LANES:]
        turn_re, turn_im = turn_ref[0], turn_ref[1]
        re, im = re * turn_re + im * turn_im, im * turn_re - re * turn_im
        re, im = column_inverse(re, im)
        for which, value in enumerate((re, im)):
            piece = (out_ref.shape[0],) + out_ref.shape[3:]
            out_ref[:, out, which] = value.reshape(piece)

    backward(0, ((2, 1), (0, 3)))
    backward(1, ((4, 1), (0, 5), (6, 3)))


def call(kernel, name, out_shapes, *args, near, scratch=()):
    spaces = [VMEM if flag else pltpu.MemorySpace.HBM for flag in near]
    args = [pltpu.with_memory_space_constraint(v, space) for v, space in zip(args, spaces)]
    specs = [pl.BlockSpec(memory_space=space) for space in spaces]
    outs = [space(shape, jnp.float32) for shape, space in zip(out_shapes, spaces[len(args) :])]
    return pl.pallas_call(
        kernel,
        out_shape=outs,
        in_specs=specs[: len(args)],
        out_specs=specs[len(args) :],
        scratch_shapes=scratch,
        compiler_params=pltpu.CompilerParams(vmem_limit_bytes=24 << 20),
        name=name,
    )(*args)


def exchange(value):
    return lax.all_to_all(value, AXES, split_axis=0, concat_axis=0, tiled=True)


def lane_tables():
    index = np.arange(LANES)
    angle = 2.0 * np.pi * ((index[:, None] * index[None, :]) % LANES) / LANES
    cos, sin = np.cos(angle), np.sin(angle)
    forward = np.block([[cos, sin], [-sin, cos]]).astype(np.float32)
    backward = np.block([[cos, -sin], [sin, cos]]).astype(np.float32)
    parts = []
    for table in (forward, backward):
        high = table.astype(jnp.bfloat16)
        low = (table - high.astype(np.float32)).astype(jnp.bfloat16)
        parts.append(np.concatenate([high, high, low], axis=0))
    return jnp.asarray(np.stack(parts))


def tables(local_limbs, devices, scaling, rate):
    rows = local_limbs // LANES
    period = 4 * local_limbs * devices
    freq = 4 * device_position() + 1

    def grid(shape):
        return (lax.broadcasted_iota(jnp.int32, shape, 0), lax.broadcasted_iota(jnp.int32, shape, 1))

    quarter = rows // 4

    def section(conjugate):
        shape = (4, quarter, quarter)
        node = lax.broadcasted_iota(jnp.int32, shape, 0)
        k = lax.broadcasted_iota(jnp.int32, shape, 2 if conjugate else 1)
        t1 = lax.broadcasted_iota(jnp.int32, shape, 1 if conjugate else 2)
        cos, sin = turn(t1 * (freq + 4 * devices * (4 * k + node)) * LANES, period)
        table = jnp.concatenate([cos, -sin if conjugate else sin], axis=1)
        high, low = split_table(table)
        return jnp.concatenate([high, high, low, low], axis=2)

    forward, backward = section(False), section(True)
    row, t2 = grid((rows, LANES))
    q1 = 4 * (row % quarter) + row // quarter
    between = jnp.stack(turn(t2 * (q1 * (period // local_limbs) + freq), period))
    spread_freq = freq + lax.broadcasted_iota(jnp.int32, (LANES,), 0) * 0
    roots = jnp.stack(turn(spread_freq, 8 * devices) + turn(spread_freq, 16 * devices))
    numer = freq + 4 * devices * (q1 + rows * t2)
    numer = jnp.where(2 * numer > period, numer - period, numer)
    angle = numer.astype(jnp.float32) * (2.0 * math.pi / period)
    half = jnp.sin(0.5 * angle)
    damp = math.exp(-rate)
    den_re = -math.expm1(-rate) + (2.0 * damp) * half * half
    den_im = -damp * jnp.sin(angle)
    norm = scaling / (den_re * den_re + den_im * den_im)
    filt = jnp.stack([den_re * norm, -den_im * norm])
    return forward, backward, between, filt, roots


def weighted_sums(received, rate):
    devices, _, piece, _ = received.shape
    shape = (devices, 1, piece, LANES)
    index = lax.broadcasted_iota(jnp.int32, shape, 2) + device_position() * piece
    index = index + lax.broadcasted_iota(jnp.int32, shape, 0) * (devices * piece)
    index = index * LANES + lax.broadcasted_iota(jnp.int32, shape, 3)
    left = devices * devices * piece * LANES - 1 - index
    return jnp.sum(received * jnp.exp(left.astype(jnp.float32) * -rate), axis=(0, 2))


def sum_over_lanes(sums):
    count = lax.axis_size("lane")
    step = 1
    while step < count:
        sums = sums + lax.ppermute(sums, "lane", [(d, d ^ step) for d in range(count)])
        step *= 2
    return sums


def group_parts(sums):
    count = lax.axis_size("grp")
    step = 1
    parts = [sums]
    while step < count:
        sums = sum(parts[1:], parts[0])
        span = min(4, count // step)
        parts = [sums] + [
            lax.ppermute(sums, "grp", [(d, d ^ (step * k)) for d in range(count)])
            for k in range(1, span)
        ]
        step *= span
    return parts


def local(*operands):
    devices = device_count()
    local_limbs = operands[0].shape[0]
    total = local_limbs * devices
    rate = 1.0 / (2 * local_limbs)
    scaling = 1.0 / (16.0 * math.sqrt(total) * math.sqrt(local_limbs))
    rows = local_limbs // LANES
    piece = rows // devices
    inside = piece % 8 == 0

    dma = pltpu.SemaphoreType.DMA
    far_ops = [v.reshape(devices, piece, LANES) for v in operands]
    (stacked,) = call(
        stack_kernel,
        "stack",
        [(devices, FWD_OPS, piece, LANES)],
        *far_ops,
        near=[False] * FWD_OPS + [True],
        scratch=[dma((FWD_OPS,))],
    )
    received = exchange(stacked)
    sums = sum_over_lanes(weighted_sums(received, rate))
    near_tables = tables(local_limbs, devices, scaling / total, rate)
    parts = group_parts(sums)
    near_consts = (*near_tables, *parts)
    lane_table = lane_tables()

    (spread,) = call(
        spread_kernel,
        "spread",
        [(devices, FWD_OPS, 2, piece, LANES)],
        received,
        near=[True, False],
        scratch=[
            pltpu.VMEM((FWD_OPS, devices, 2, piece, LANES), jnp.float32),
            dma((FWD_OPS,)),
        ],
    )
    landed = exchange(spread)
    if not inside:
        landed = landed.transpose(1, 2, 0, 3, 4).reshape(1, FWD_OPS, 2, rows, LANES)
    (turned,) = call(
        functools.partial(spectrum_kernel, damp=math.exp(-rate)),
        "spectrum",
        [(devices, 2, 2, piece, LANES) if inside else (1, 2, 2, rows, LANES)],
        landed,
        *near_consts,
        lane_table,
        near=[True] * (1 + len(near_consts)) + [False, True],
        scratch=[
            pltpu.VMEM((FWD_OPS, rows, 2 * LANES), jnp.float32),
            pltpu.VMEM((FWD_OPS, rows, 6 * LANES), jnp.bfloat16),
            pltpu.VMEM(lane_table.shape, lane_table.dtype),
            dma((1,)),
        ],
    )
    if not inside:
        turned = turned.reshape(2, 2, devices, piece, LANES).transpose(2, 0, 1, 3, 4)
    gathered = exchange(turned)
    (coeffs,) = call(
        gather_kernel, "gather", [(devices, 2, 2, piece, LANES)], gathered, near=[True] * 2
    )
    owned = exchange(coeffs)
    results = call(
        deliver_kernel,
        "deliver",
        [(2, devices, piece, LANES)] * 2,
        owned,
        near=[True, False, False],
        scratch=[dma((4,))],
    )
    return tuple(v.reshape(2 * local_limbs) for v in results)


def solution(mesh):
    return jax.shard_map(
        local,
        mesh=mesh,
        in_specs=(P(AXES),) * FWD_OPS,
        out_specs=(P(AXES), P(AXES)),
        check_vma=False,
    )
```

```python
import functools
import math

import jax
import jax.numpy as jnp
import numpy as np
from jax import lax
from jax.experimental import pallas as pl
from jax.experimental.pallas import tpu as pltpu
from jax.sharding import PartitionSpec as P

AXES = ("grp", "lane")
LANES = 128
FWD_OPS = 7
VMEM = pltpu.MemorySpace.VMEM


def device_count():
    return lax.axis_size("grp") * lax.axis_size("lane")


def device_position():
    return lax.axis_index("grp") * lax.axis_size("lane") + lax.axis_index("lane")


def turn(numer, denom):
    reduced = numer % denom
    reduced = jnp.where(2 * reduced > denom, reduced - denom, reduced)
    angle = reduced.astype(jnp.float32) * (2.0 * math.pi / denom)
    return jnp.cos(angle), jnp.sin(angle)


def split16(value):
    high = value.astype(jnp.bfloat16)
    return high, (value - high.astype(jnp.float32)).astype(jnp.bfloat16)


def split_table(value):
    high = lax.reduce_precision(value, 8, 7)
    return high.astype(jnp.bfloat16), (value - high).astype(jnp.bfloat16)


def wide_left(parts):
    return jnp.concatenate([parts[0], parts[1], parts[0]], axis=1)


def tall_right(parts):
    return jnp.concatenate([parts[0], parts[0], parts[1]], axis=0)


def dot32(left, right):
    return jnp.dot(left, right, preferred_element_type=jnp.float32)


def tree_forward(values, numer, denom, emit):
    if len(values) == 1:
        emit(numer, denom, values[0])
        return
    half = len(values) // 2
    numer, denom = numer, 2 * denom
    cos, sin = math.cos(2 * math.pi * numer / denom), math.sin(2 * math.pi * numer / denom)
    plus, minus = [], []
    for low, high in zip(values[:half], values[half:]):
        if low[1] is None:
            re, im = cos * high[0], sin * high[0]
            plus.append((low[0] + re, im))
            minus.append((low[0] - re, -im))
        else:
            re = cos * high[0] - sin * high[1]
            im = sin * high[0] + cos * high[1]
            plus.append((low[0] + re, low[1] + im))
            minus.append((low[0] - re, low[1] - im))
    tree_forward(plus, numer, denom, emit)
    tree_forward(minus, numer + denom // 2, denom, emit)


def tree_inverse(size, numer, denom, load):
    if size == 1:
        return [load(numer, denom)]
    denom = 2 * denom
    cos, sin = math.cos(2 * math.pi * numer / denom), math.sin(2 * math.pi * numer / denom)
    plus = tree_inverse(size // 2, numer, denom, load)
    minus = tree_inverse(size // 2, numer + denom // 2, denom, load)
    low = [(a[0] + b[0], a[1] + b[1]) for a, b in zip(plus, minus)]
    high = []
    for a, b in zip(plus, minus):
        re, im = a[0] - b[0], a[1] - b[1]
        high.append((cos * re + sin * im, cos * im - sin * re))
    return low + high


def slot_of(numer, denom, devices):
    numer = (numer * (4 * devices // denom)) % (4 * devices)
    return (numer - 1) // 4


def spread_kernel(x_ref, out_far, out_ref, sems):
    devices = x_ref.shape[0]
    copies = []
    for op in range(FWD_OPS):
        values = [(x_ref[d, op], None) for d in range(devices)]

        def emit(numer, denom, value):
            slot = slot_of(numer, denom, devices)
            out_ref[op, slot, 0] = value[0]
            out_ref[op, slot, 1] = value[1]

        tree_forward(values, 1, 4, emit)
        copies.append(pltpu.make_async_copy(out_ref.at[op], out_far.at[:, op], sems.at[op]))
        copies[-1].start()
    for copy in copies:
        copy.wait()


def gather_kernel(u_ref, out_ref):
    devices = u_ref.shape[0]
    for out in range(2):

        def load(numer, denom):
            slot = slot_of(numer, denom, devices)
            return u_ref[slot, out, 0], u_ref[slot, out, 1]

        for block, pair in enumerate(tree_inverse(devices, 1, 4, load)):
            for k, value in enumerate(pair):
                index = k * devices + block
                out_ref[index // 2, out, index % 2] = value


def copy_all(pairs, sems):
    copies = [pltpu.make_async_copy(a, b, sems.at[k]) for k, (a, b) in enumerate(pairs)]
    for copy in copies:
        copy.start()
    return copies


def stack_kernel(*refs):
    operands, out_ref, sems = refs[:-2], refs[-2], refs[-1]
    pairs = [(ref, out_ref.at[:, op]) for op, ref in enumerate(operands)]
    for copy in copy_all(pairs, sems):
        copy.wait()


def deliver_kernel(in_ref, first_ref, second_ref, sems):
    pairs = [
        (in_ref.at[:, out, half], ref.at[half])
        for out, ref in enumerate((first_ref, second_ref))
        for half in range(2)
    ]
    for copy in copy_all(pairs, sems):
        copy.wait()


def spectrum_kernel(x_ref, a_ref, ai_ref, turn_ref, h_ref, roots_ref, *rest, damp):
    totals_refs, (b_far, out_ref, spec_ref, lhs_ref, b_ref, sems) = rest[:-6], rest[-6:]
    rows = turn_ref.shape[1]
    copies = copy_all([(b_far, b_ref)], sems)

    quarter = rows // 4
    rho = (roots_ref[0:1], roots_ref[1:2])
    sigma = (roots_ref[2:3], roots_ref[3:4])

    def times(a, b):
        return a[0] * b[0] - a[1] * b[1], a[0] * b[1] + a[1] * b[0]

    def times_conj(a, b):
        return a[0] * b[0] + a[1] * b[1], a[1] * b[0] - a[0] * b[1]

    def add(a, b):
        return a[0] + b[0], a[1] + b[1]

    def sub(a, b):
        return a[0] - b[0], a[1] - b[1]

    def section(table, value):
        high, low = split16(jnp.concatenate(value, axis=1))
        both = dot32(table, jnp.concatenate([high, low, high, low], axis=0))
        top, bottom = both[:quarter], both[quarter:]
        return top[:, :LANES] - bottom[:, LANES:], top[:, LANES:] + bottom[:, :LANES]

    def join(values):
        return tuple(jnp.concatenate([v[k] for v in values], axis=0) for k in range(2))

    def cut(re, im):
        parts = [slice(m * quarter, (m + 1) * quarter) for m in range(4)]
        return [(re[part], im[part]) for part in parts]

    def column_forward(re, im):
        x = cut(re, im)
        turned = [times(x[2], rho), times(x[3], rho)]
        plus = [add(x[0], turned[0]), add(x[1], turned[1])]
        minus = [sub(x[0], turned[0]), sub(x[1], turned[1])]
        even, odd = times(plus[1], sigma), times(minus[1], sigma)
        odd = (-odd[1], odd[0])
        nodes = [add(plus[0], even), add(minus[0], odd), sub(plus[0], even), sub(minus[0], odd)]
        return join([section(a_ref[j], nodes[j]) for j in range(4)])

    def column_inverse(re, im):
        nodes = [section(ai_ref[j], value) for j, value in enumerate(cut(re, im))]
        odd = sub(nodes[1], nodes[3])
        plus = [add(nodes[0], nodes[2]), times_conj(sub(nodes[0], nodes[2]), sigma)]
        minus = [add(nodes[1], nodes[3]), times_conj((odd[1], -odd[0]), sigma)]
        low = [add(plus[m], minus[m]) for m in range(2)]
        high = [times_conj(sub(plus[m], minus[m]), rho) for m in range(2)]
        return join(low + high)

    def forward(first, last):
        for op in range(first, last):
            re, im = column_forward(
                x_ref[:, op, 0].reshape(rows, LANES), x_ref[:, op, 1].reshape(rows, LANES)
            )
            turn_re, turn_im = turn_ref[0], turn_ref[1]
            turned = jnp.concatenate(
                [re * turn_re - im * turn_im, re * turn_im + im * turn_re], axis=1
            )
            lhs_ref[op] = wide_left(split16(turned))
        if first == 0:
            copies[0].wait()
        count = last - first
        left = lhs_ref[first:last].reshape(count * rows, lhs_ref.shape[2])
        spec_ref[first:last] = dot32(left, b_ref[0]).reshape(count, rows, 2 * LANES)

    forward(0, 4)
    forward(4, FWD_OPS)

    totals = sum(ref[...] for ref in totals_refs)
    totals = damp * jnp.sum(totals, axis=1, keepdims=True)

    def member(op):
        return spec_ref[op, :, :LANES], spec_ref[op, :, LANES:]

    def products(pairs):
        re, im = 0.0, 0.0
        for left, right in pairs:
            left_re, left_im = member(left)
            right_re, right_im = member(right)
            re = re + (left_re * right_re - left_im * right_im)
            im = im + (left_re * right_im + left_im * right_re)
        return re, im

    damped = []
    for pairs in (((2, 1), (0, 3)), ((4, 1), (0, 5), (6, 3))):
        re, im = products(pairs)
        re = re + sum(totals[a : a + 1] * totals[b : b + 1] for a, b in pairs)
        value = times((re, im), (h_ref[0], h_ref[1]))
        damped.append(wide_left(split16(jnp.concatenate(value, axis=1))))
    both = dot32(jnp.concatenate(damped, axis=0), b_ref[1])
    for out in range(2):
        part = both[out * rows : (out + 1) * rows]
        value = times_conj((part[:, :LANES], part[:, LANES:]), (turn_ref[0], turn_ref[1]))
        for which, value in enumerate(column_inverse(*value)):
            piece = (out_ref.shape[0],) + out_ref.shape[3:]
            out_ref[:, out, which] = value.reshape(piece)


def call(kernel, name, out_shapes, *args, near, scratch=()):
    spaces = [VMEM if flag else pltpu.MemorySpace.HBM for flag in near]
    args = [pltpu.with_memory_space_constraint(v, space) for v, space in zip(args, spaces)]
    specs = [pl.BlockSpec(memory_space=space) for space in spaces]
    outs = [space(shape, jnp.float32) for shape, space in zip(out_shapes, spaces[len(args) :])]
    return pl.pallas_call(
        kernel,
        out_shape=outs,
        in_specs=specs[: len(args)],
        out_specs=specs[len(args) :],
        scratch_shapes=scratch,
        compiler_params=pltpu.CompilerParams(vmem_limit_bytes=24 << 20),
        name=name,
    )(*args)


def exchange(value):
    return lax.all_to_all(value, AXES, split_axis=0, concat_axis=0, tiled=True)


def lane_tables():
    index = np.arange(LANES)
    angle = 2.0 * np.pi * ((index[:, None] * index[None, :]) % LANES) / LANES
    cos, sin = np.cos(angle), np.sin(angle)
    forward = np.block([[cos, sin], [-sin, cos]]).astype(np.float32)
    backward = np.block([[cos, -sin], [sin, cos]]).astype(np.float32)
    parts = []
    for table in (forward, backward):
        high = table.astype(jnp.bfloat16)
        low = (table - high.astype(np.float32)).astype(jnp.bfloat16)
        parts.append(np.concatenate([high, high, low], axis=0))
    return jnp.asarray(np.stack(parts))


def tables(local_limbs, devices, scaling, rate):
    rows = local_limbs // LANES
    period = 4 * local_limbs * devices
    freq = 4 * device_position() + 1

    def grid(shape):
        return (lax.broadcasted_iota(jnp.int32, shape, 0), lax.broadcasted_iota(jnp.int32, shape, 1))

    quarter = rows // 4

    def section(conjugate):
        shape = (4, quarter, quarter)
        node = lax.broadcasted_iota(jnp.int32, shape, 0)
        k = lax.broadcasted_iota(jnp.int32, shape, 2 if conjugate else 1)
        t1 = lax.broadcasted_iota(jnp.int32, shape, 1 if conjugate else 2)
        cos, sin = turn(t1 * (freq + 4 * devices * (4 * k + node)) * LANES, period)
        table = jnp.concatenate([cos, -sin if conjugate else sin], axis=1)
        high, low = split_table(table)
        return jnp.concatenate([high, high, low, low], axis=2)

    forward, backward = section(False), section(True)
    row, t2 = grid((rows, LANES))
    q1 = 4 * (row % quarter) + row // quarter
    between = jnp.stack(turn(t2 * (q1 * (period // local_limbs) + freq), period))
    spread_freq = freq + lax.broadcasted_iota(jnp.int32, (LANES,), 0) * 0
    roots = jnp.stack(turn(spread_freq, 8 * devices) + turn(spread_freq, 16 * devices))
    numer = freq + 4 * devices * (q1 + rows * t2)
    numer = jnp.where(2 * numer > period, numer - period, numer)
    angle = numer.astype(jnp.float32) * (2.0 * math.pi / period)
    half = jnp.sin(0.5 * angle)
    damp = math.exp(-rate)
    den_re = -math.expm1(-rate) + (2.0 * damp) * half * half
    den_im = -damp * jnp.sin(angle)
    norm = scaling / (den_re * den_re + den_im * den_im)
    filt = jnp.stack([den_re * norm, -den_im * norm])
    return forward, backward, between, filt, roots


def weighted_sums(received, rate):
    devices, _, piece, _ = received.shape
    shape = (devices, 1, piece, LANES)
    index = lax.broadcasted_iota(jnp.int32, shape, 2) + device_position() * piece
    index = index + lax.broadcasted_iota(jnp.int32, shape, 0) * (devices * piece)
    index = index * LANES + lax.broadcasted_iota(jnp.int32, shape, 3)
    left = devices * devices * piece * LANES - 1 - index
    return jnp.sum(received * jnp.exp(left.astype(jnp.float32) * -rate), axis=(0, 2))


def sum_over_lanes(sums):
    count = lax.axis_size("lane")
    step = 1
    while step < count:
        sums = sums + lax.ppermute(sums, "lane", [(d, d ^ step) for d in range(count)])
        step *= 2
    return sums


def group_parts(sums):
    count = lax.axis_size("grp")
    step = 1
    parts = [sums]
    while step < count:
        sums = sum(parts[1:], parts[0])
        span = min(4, count // step)
        parts = [sums] + [
            lax.ppermute(sums, "grp", [(d, d ^ (step * k)) for d in range(count)])
            for k in range(1, span)
        ]
        step *= span
    return parts


def local(*operands):
    devices = device_count()
    local_limbs = operands[0].shape[0]
    total = local_limbs * devices
    rate = 1.0 / (2 * local_limbs)
    scaling = 1.0 / (16.0 * math.sqrt(total) * math.sqrt(local_limbs))
    rows = local_limbs // LANES
    piece = rows // devices
    inside = piece % 8 == 0

    dma = pltpu.SemaphoreType.DMA
    far_ops = [v.reshape(devices, piece, LANES) for v in operands]
    (stacked,) = call(
        stack_kernel,
        "stack",
        [(devices, FWD_OPS, piece, LANES)],
        *far_ops,
        near=[False] * FWD_OPS + [True],
        scratch=[dma((FWD_OPS,))],
    )
    received = exchange(stacked)
    sums = sum_over_lanes(weighted_sums(received, rate))
    near_tables = tables(local_limbs, devices, scaling / total, rate)
    parts = group_parts(sums)
    near_consts = (*near_tables, *parts)
    lane_table = lane_tables()

    (spread,) = call(
        spread_kernel,
        "spread",
        [(devices, FWD_OPS, 2, piece, LANES)],
        received,
        near=[True, False],
        scratch=[
            pltpu.VMEM((FWD_OPS, devices, 2, piece, LANES), jnp.float32),
            dma((FWD_OPS,)),
        ],
    )
    landed = exchange(spread)
    if not inside:
        landed = landed.transpose(1, 2, 0, 3, 4).reshape(1, FWD_OPS, 2, rows, LANES)
    (turned,) = call(
        functools.partial(spectrum_kernel, damp=math.exp(-rate)),
        "spectrum",
        [(devices, 2, 2, piece, LANES) if inside else (1, 2, 2, rows, LANES)],
        landed,
        *near_consts,
        lane_table,
        near=[True] * (1 + len(near_consts)) + [False, True],
        scratch=[
            pltpu.VMEM((FWD_OPS, rows, 2 * LANES), jnp.float32),
            pltpu.VMEM((FWD_OPS, rows, 6 * LANES), jnp.bfloat16),
            pltpu.VMEM(lane_table.shape, lane_table.dtype),
            dma((1,)),
        ],
    )
    if not inside:
        turned = turned.reshape(2, 2, devices, piece, LANES).transpose(2, 0, 1, 3, 4)
    gathered = exchange(turned)
    (coeffs,) = call(
        gather_kernel, "gather", [(devices, 2, 2, piece, LANES)], gathered, near=[True] * 2
    )
    owned = exchange(coeffs)
    results = call(
        deliver_kernel,
        "deliver",
        [(2, devices, piece, LANES)] * 2,
        owned,
        near=[True, False, False],
        scratch=[dma((4,))],
    )
    return tuple(v.reshape(2 * local_limbs) for v in results)


def solution(mesh):
    return jax.shard_map(
        local,
        mesh=mesh,
        in_specs=(P(AXES),) * FWD_OPS,
        out_specs=(P(AXES), P(AXES)),
        check_vma=False,
    )
```
